32 devices in a mesh: slab: 4 (over y, x), sta: 8 (over z, core).
Axes of the slice: x: 2, y: 2, z: 4, core: 2. Of those that a mesh axis runs over, the one named last changes fastest.
Arguments:
- station_place: float32 [32, 2], P('sta'), may hold values from 0 to 1
- station_height: float32 [32], P('sta'), may hold values from 2 to 8
- cell_weight: float32 [256, 256, 64], P('slab'), may hold values from 0.5 to 2
- kept: int32 [4, 32, 16], P('slab', 'sta'), may hold values from 0 to 8191, as said below
- dest: int32 [4, 32, 16, 1], P('slab', 'sta'), may hold values from 0 to 7; in each aligned block of 64 rows (0 to 63, 64 to 127, ..., all dimensions but the last counted through in order) at most 24 rows name the same one
Outputs:
- owned_blocks: float32 [4, 8, 8, 24, 128], P('slab', 'sta')
The draws below stay inside these ranges and needn't reach their ends.
Inputs may be any that keep to these rules, and one draw needn't show every extreme that they name: `dest`: in the rows of one device (aligned blocks of 64 rows, in order), each owner is named by at most 24 rows, a bound that some block reaches. Let a = k // (256 / (2 * 4)) for a kept id k, and let x-slab p hold x from p * 256 / 4 on, 256 / 4 of them. When a >= 4, the cells on which row a of H(256) is nonzero lie in one x-slab. Among the 64 ids of one y-slab and one index of sta, at most 32 ids with a >= 4 touch any one x-slab, and some x-slab is touched by exactly 32.
All inputs are finite; a program needn't handle non-finite values.
Results may differ from the reference program's by a relative error of at most 0.0003.
Values sent between devices are 32-bit elements; how exact they have to be, the bound alone decides.
A program may use at most 128 MiB of HBM per device.

```python
import math
import jax
import jax.numpy as jnp
import numpy as np
from jax import lax

NX = 256
NY = 256
NZ = 64
STA_DEV = 4
KEEP = 16
STATIONS = 32
CAP = 24
N_SLAB = 4
N_STA = 8


def fine_row(slab, chosen):
    x_local = NX // N_SLAB
    result = jnp.zeros_like(chosen)
    base = 0
    width = 2
    while width <= x_local:
        count = x_local // width
        inside = (chosen >= base) & (chosen < base + count)
        result = jnp.where(inside, NX // width + slab * count + chosen - base, result)
        base = base + count
        width = width * 2
    return result


def draw_kept(key, part):
    rows = STA_DEV * KEEP
    half = NY // N_SLAB // 2
    x_local = NX // N_SLAB
    limit = max(2, 2 * rows // N_SLAB)
    classes = N_SLAB + 1

    def one_group(sub):
        keys = jax.random.split(sub, 6)
        full_slab = jax.random.randint(keys[0], (), 0, N_SLAB)
        shuffled = jax.random.permutation(keys[1], classes * limit)
        class_of = (shuffled // limit).astype(jnp.int32)
        score = jnp.where(class_of == full_slab, 0, 1 + jnp.arange(classes * limit, dtype=jnp.int32))
        ordered = class_of[jnp.argsort(score, stable=True)]
        taken = jax.random.permutation(keys[2], ordered[:rows])
        chosen = jax.random.randint(keys[3], (rows,), 0, x_local - 1)
        fine = fine_row(jnp.minimum(taken, N_SLAB - 1), chosen)
        coarse = jax.random.randint(keys[4], (rows,), 0, N_SLAB)
        xrows = jnp.where(taken == N_SLAB, coarse, fine)
        pairs = jax.random.randint(keys[5], (rows,), 0, half)
        return (xrows * half + pairs).astype(jnp.int32)
    groups = jax.random.split(jax.random.fold_in(key, 71), N_SLAB * N_STA)
    table = jax.vmap(one_group)(groups)
    return table.reshape(N_SLAB, N_STA * STA_DEV, KEEP)


def levels(own_key, extent, pieces, least, high):
    def one(dim, parts):
        draws = jax.random.uniform(jax.random.fold_in(jax.random.fold_in(own_key, 6), dim), (parts,), jnp.float32, least / len(pieces), high / len(pieces))
        return jnp.repeat(jnp.exp(draws), extent[dim] // parts).reshape((-1,) + (1,) * (len(extent) - dim - 1))

    level = one(*pieces[0])
    for cut in pieces[1:]:
        level = level * one(*cut)
    return level


def shared_out(key, own, number, rows, number_of, top, reach, skew):
    ranking = jax.random.permutation(key, number_of)
    packed, common = load_shares(number_of, rows * top, reach, skew, True), load_shares(number_of, rows * top, reach, skew, False)
    places = jnp.arange(number_of)

    def named(lengths, turn):
        used = int((lengths > 0).sum())
        fixed = max(1, used // 4)
        passed = fixed + (places - fixed + turn * (used - fixed)) % max(1, number_of - fixed)
        return jnp.zeros((number_of,), jnp.int32).at[ranking[jnp.where(places < fixed, places, passed)]].set(jnp.asarray(lengths, jnp.int32))

    lengths = jnp.where(number % 4 == 0, named(packed, number // 4), named(common, number - number // 4 - 1))
    mixed = jax.random.permutation(jax.random.fold_in(own, 3), number_of)
    donor, sink = mixed[0:number_of // 2 * 2:2], mixed[1:number_of // 2 * 2:2]
    margin = jnp.minimum(lengths[donor] - 1, reach - lengths[sink]) // 2
    margin = jnp.where((donor == ranking[0]) | (sink == ranking[0]) | (lengths[sink] == 0), 0, jnp.maximum(margin, 0))
    passed = jax.random.randint(jax.random.fold_in(own, 4), (number_of // 2,), 0, 1 << 20) % (margin + 1)
    lengths = lengths.at[donor].add(-passed).at[sink].add(passed)
    members = jnp.searchsorted(jnp.cumsum(lengths), jnp.arange(rows * top), side="right").astype(jnp.int32)
    grid = members.reshape(top, rows).T
    grid = grid[jax.random.permutation(jax.random.fold_in(own, 1), rows)]
    turn = jax.random.randint(jax.random.fold_in(own, 2), (rows, 1), 0, top)
    return jnp.take_along_axis(grid, (jnp.arange(top)[None, :] + turn) % top, axis=1)


def load_shares(number_of, total, most, skew, full):
    weights = [(1 << 20) // math.isqrt(standing ** skew) + 1 for standing in range(1, number_of + 1)]
    largest = most if full else min(most, max(-(-total // number_of), total * weights[0] // sum(weights)))
    least = 1 if total - largest >= number_of - 1 else 0
    holding, surplus = [largest] + [least] * (number_of - 1), total - largest - least * (number_of - 1)
    while surplus > 0:
        free = [i for i in range(1, number_of) if holding[i] < largest] or [i for i in range(1, number_of) if holding[i] < most]
        pool, budget = sum([weights[i] for i in free]), surplus
        for i in free:
            more = min(most - holding[i], max(1, budget * weights[i] // pool), surplus)
            holding[i] = holding[i] + more
            surplus = surplus - more
    return np.array(holding)


def setup_inputs(seed: int = 0) -> dict:
    streams_of = jax.random.split(jax.random.key(seed), 6)
    station_place = jnp.clip(1.0 * jax.random.uniform(streams_of[0], (STATIONS, 2), jnp.float32) ** levels(streams_of[0], (STATIONS, 2), ((0, 8),), -0.2, 0.2), 0.0, 1.0)
    station_height = jnp.clip(jnp.exp(math.log(8.0) - 1.3862944 * jax.random.uniform(streams_of[1], (STATIONS,), jnp.float32) ** levels(streams_of[1], (STATIONS,), ((0, 8),), -0.2, 0.2)), 2.0, 8.0)
    cell_weight = jnp.clip(jnp.exp(math.log(2.0) - 1.3862944 * jax.random.uniform(streams_of[2], (NX, NY, NZ), jnp.float32) ** levels(streams_of[2], (NX, NY, NZ), ((0, 4),), -0.2, 0.2)), 0.5, 2.0)
    kept = draw_kept(jax.random.fold_in(streams_of[5], 71), 0)
    dest_keys = jax.random.split(jax.random.fold_in(streams_of[4], 1), N_SLAB * STATIONS * KEEP // (STA_DEV * KEEP))
    dest_turns = jax.random.permutation(jax.random.fold_in(streams_of[4], 3), N_SLAB * STATIONS * KEEP // (STA_DEV * KEEP))
    dest = jax.vmap(lambda own, number: shared_out(jax.random.fold_in(streams_of[4], 2), own, number, STA_DEV * KEEP, N_STA, 1, CAP, 2))(dest_keys, dest_turns).reshape((N_SLAB, STATIONS, KEEP, 1))
    return dict(station_place=station_place, station_height=station_height, cell_weight=cell_weight, kept=kept, dest=dest)


kernel_scale = 32.0
root_half = 0.7071067811865476

def haar(order):
    matrix = jnp.eye(order, dtype=jnp.float32)
    rows = jnp.arange(order, dtype=jnp.int32)[:, None]
    cols = jnp.arange(order, dtype=jnp.int32)[None, :]
    active = order
    while active % 2 == 0 and active > 1:
        half = active // 2
        low = (rows < half) & ((cols == 2 * rows) | (cols == 2 * rows + 1))
        upper = (rows >= half) & (rows < active)
        plus = upper & (cols == 2 * (rows - half))
        minus = upper & (cols == 2 * (rows - half) + 1)
        keeps = (rows >= active) & (rows == cols)
        step = (jnp.where(low | plus, root_half, 0.0) - jnp.where(minus, root_half, 0.0) + jnp.where(keeps, 1.0, 0.0)).astype(jnp.float32)
        matrix = jnp.dot(step, matrix, precision=lax.Precision.HIGHEST, preferred_element_type=jnp.float32)
        active = half
    return matrix

def kernel(place, height, weight, xs, nx, ny, nz):
    ys = jnp.arange(ny, dtype=jnp.int32).astype(jnp.float32) + 0.5
    zs = jnp.arange(nz, dtype=jnp.int32).astype(jnp.float32) + 0.5
    east = xs[None, :] - place[:, 0:1] * nx
    north = ys[None, :] - place[:, 1:2] * ny
    depth = zs[None, :] + height[:, None]
    radius = east[:, :, None, None] ** 2 + north[:, None, :, None] ** 2 + depth[:, None, None, :] ** 2
    return kernel_scale * weight[None] * depth[:, None, None, :] / (radius * jnp.sqrt(radius))

def reference(station_place, station_height, cell_weight, kept, dest):
    wx, wy, wz = (haar(NX), haar(NY), haar(NZ))
    half = NY // N_SLAB // 2
    xs = jnp.arange(NX, dtype=jnp.int32).astype(jnp.float32) + 0.5
    slabs = jnp.arange(N_SLAB, dtype=jnp.int32)[:, None]

    def one(item):
        place, height, ids = item
        field = kernel(place[None], height[None], cell_weight, xs, NX, NY, NZ)[0]
        field = jnp.einsum('xyz,cz->xyc', field, wz, precision=lax.Precision.HIGHEST)
        field = jnp.einsum('by,xyc->xbc', wy, field, precision=lax.Precision.HIGHEST)
        paired = field.reshape(NX, NY // 2, 2 * NZ)
        xrow = (ids // half).reshape(-1)
        ypair = (slabs * half + ids % half).reshape(-1)
        gathered = paired[:, ypair, :]
        weights = wx[xrow]
        blocks = jnp.einsum('mx,xmc->mc', weights, gathered, precision=lax.Precision.HIGHEST)
        return blocks.reshape(N_SLAB, KEEP, 2 * NZ)
    blocks = lax.map(one, (station_place, station_height, jnp.transpose(kept, (1, 0, 2))))
    per_row = STA_DEV * KEEP
    values = jnp.transpose(blocks, (1, 0, 2, 3)).reshape(N_SLAB, N_STA, per_row, 2 * NZ)
    owner = dest.reshape(N_SLAB, N_STA, per_row)
    owners = jnp.arange(N_STA, dtype=jnp.int32)
    onehot = (owner[..., None] == owners).astype(jnp.int32)
    slot = lax.optimization_barrier(jnp.sum((jnp.cumsum(onehot, axis=2) - onehot) * onehot, axis=3)).astype(jnp.int32)
    slab_ids = jnp.arange(N_SLAB, dtype=jnp.int32)[:, None, None]
    source = jnp.arange(N_STA, dtype=jnp.int32)[None, :, None]
    result = jnp.zeros((N_SLAB, N_STA, N_STA, CAP, 2 * NZ), jnp.float32)
    return result.at[slab_ids, owner, source, slot].set(values)
```

```python
import functools

import jax
import jax.numpy as jnp
from jax import lax
from jax.experimental import pallas as pl
from jax.experimental.pallas import tpu as pltpu
from jax.sharding import PartitionSpec as P

kernel_scale = 32.0
MESH = pl.DeviceIdType.MESH


def log2(n):
    return n.bit_length() - 1


def pyramid(pairs, level):
    return 2 * pairs - (2 * pairs >> level)


def row_plan(ids, j, me, slab, half, x_cells, y_cells):
    ls = log2(slab)
    pairs = x_cells // slab // 2
    a = ids >> log2(half)
    pair = j * half + (ids & (half - 1))
    total = pyramid(pairs, log2(pairs))
    first = jnp.full(a.shape, total, jnp.int32)
    second = jnp.full(a.shape, total, jnp.int32)
    factor = jnp.full(a.shape, x_cells ** -0.5, jnp.float32)
    turn = jnp.full(a.shape, 1.0, jnp.float32)
    back = jnp.full(a.shape, 0.0, jnp.float32)
    m = 1
    while m < x_cells:
        e = log2(m)
        at = a >= m
        k = a - m
        norm = (m / x_cells) ** 0.5
        if m >= slab:
            sh = e - ls
            mine = (k >> sh) == me
            here = k & ((1 << sh) - 1)
            factor = jnp.where(at, jnp.where(mine, norm, 0.0), factor)
            width = x_cells // m
            if width == 2:
                first = jnp.where(at, here, first)
                second = jnp.where(at, here, second)
                turn = jnp.where(at, -1.0, turn)
                back = jnp.where(at, 0.0, back)
            else:
                off = pyramid(pairs, log2(width) - 2)
                first = jnp.where(at, off + 2 * here, first)
                second = jnp.where(at, off + 2 * here + 1, second)
                back = jnp.where(at, -1.0, back)
        else:
            sh = ls - e
            mine = k == (me >> sh)
            sign = norm * (1 - 2 * ((me >> (sh - 1)) & 1)).astype(jnp.float32)
            factor = jnp.where(at, jnp.where(mine, sign, 0.0), factor)
        m = m * 2
    ynorm = jnp.full(a.shape, y_cells ** -0.5, jnp.float32)
    m = 1
    while m < y_cells // 2:
        ynorm = jnp.where(pair >= m, (2 * m / y_cells) ** 0.5, ynorm)
        m = m * 2

    def address(row):
        at = ((row & ~7) + pair) * y_cells + (row & 7)
        m = 16
        while m < y_cells:
            k = 2 * pair - m
            wide = m // 8
            spot = 8 * (wide + (k & (wide - 1))) + (k >> log2(wide))
            at = jnp.where(k >= 0, row * y_cells + spot, at)
            m = m * 2
        return at

    factor = factor * ynorm
    return address(first), address(second), factor, factor * turn, back


def z_matrix(z_cells, t):
    z = lax.broadcasted_iota(jnp.int32, (2 * z_cells, 2 * z_cells), 0) & (z_cells - 1)
    lane = lax.broadcasted_iota(jnp.int32, (2 * z_cells, 2 * z_cells), 1)
    c = lane & (z_cells - 1)
    value = jnp.full(z.shape, z_cells ** -0.5, jnp.float32)
    m = 1
    while m < z_cells:
        w = log2(z_cells // m)
        k = c - m
        norm = (m / z_cells) ** 0.5
        hit = (z >> w) == k
        up = ((z >> (w - 1)) & 1) == 0
        value = jnp.where(c >= m, jnp.where(hit, jnp.where(up, norm, -norm), 0.0), value)
        m = m * 2
    return jnp.where((lane >> log2(z_cells)) == t, value, 0.0)


def tree(values):
    out = [None] * len(values)
    while len(values) > 1:
        half = len(values) // 2
        for k in range(half):
            out[half + k] = values[2 * k] - values[2 * k + 1]
        values = [values[2 * k] + values[2 * k + 1] for k in range(half)]
    out[0] = values[0]
    return out


GROUP = 4
CHUNK = 8


def whole_kernel(
    sizes, place, height, w_hbm, kept, dest, out,
    field, sums, halves, weights, turned, table, select, others, rows_v, rows_s, scale_v, back_v,
    taken, given, parts, arrived, packed,
    w_sem, row_sem, i_send, i_recv, s_send, s_recv, o_send, o_recv, own_sem,
):
    slab, owners, stations, keep, x_local, y_cells, z_cells, capacity = sizes
    lanes = 2 * z_cells
    pairs = x_local // 2
    rows_x = 2 * pairs
    groups = pairs // GROUP
    chunks = x_local // CHUNK
    x_cells = x_local * slab
    half = y_cells // slab // 2
    per_row = stations * keep
    runs = y_cells // 8
    me, q = lax.axis_index("slab"), lax.axis_index("sta")
    plane = rows_x * y_cells
    left = lax.broadcasted_iota(jnp.int32, (8, lanes), 1) < z_cells
    zed = (lax.broadcasted_iota(jnp.int32, (8, lanes), 1) & (z_cells - 1)).astype(jnp.float32) + 0.5
    beside = jnp.where(left, 0.5, 1.5)

    def before(d):
        return lax.rem(me - d + slab, slab)

    def id_copy(d):
        return pltpu.make_async_remote_copy(
            src_ref=kept.at[0],
            dst_ref=others.at[d - 1],
            send_sem=i_send.at[d - 1],
            recv_sem=i_recv.at[d - 1],
            device_id=(lax.rem(me + d, slab), q),
            device_id_type=MESH,
        )

    def part_copy(d):
        return pltpu.make_async_remote_copy(
            src_ref=parts.at[d],
            dst_ref=arrived.at[d - 1],
            send_sem=s_send.at[d - 1],
            recv_sem=s_recv.at[d - 1],
            device_id=(before(d), q),
            device_id_type=MESH,
        )

    def out_copy(d):
        to = lax.rem(q + d, owners)
        return pltpu.make_async_remote_copy(
            src_ref=packed.at[to],
            dst_ref=out.at[q],
            send_sem=o_send.at[d - 1],
            recv_sem=o_recv.at[d - 1],
            device_id=(me, to),
            device_id_type=MESH,
        )

    def row_copy():
        return pltpu.make_async_copy(rows_v, rows_s, row_sem)

    def w_copy(c):
        return pltpu.make_async_copy(
            w_hbm.at[pl.ds(c * CHUNK, CHUNK)], weights.at[pl.ds(c * CHUNK, CHUNK)], w_sem.at[c]
        )

    for c in range(chunks):
        w_copy(c).start()
    barrier = pltpu.get_barrier_semaphore()
    for d in range(1, slab):
        pl.semaphore_signal(
            barrier, inc=1, device_id=(lax.rem(me + d, slab), q), device_id_type=MESH
        )
    for d in range(1, owners):
        pl.semaphore_signal(
            barrier, inc=1, device_id=(me, lax.rem(q + d, owners)), device_id_type=MESH
        )

    base = (lax.broadcasted_iota(jnp.int32, (8, lanes), 0) * runs).astype(jnp.float32) + 0.5
    for s in range(stations):
        depth = zed + height[s]
        square = depth * depth
        north = base - place[1, s] * y_cells
        for r in range(runs):
            n = north + float(r)
            table[s, r] = n * n + square
    owner = jnp.zeros((1, per_row), jnp.float32)
    for s in range(stations):
        spread = lax.broadcasted_iota(jnp.int32, (keep, per_row), 1) == (
            lax.broadcasted_iota(jnp.int32, (keep, per_row), 0) + s * keep
        )
        owner = owner + jnp.dot(
            dest[s].astype(jnp.float32), spread.astype(jnp.float32),
            preferred_element_type=jnp.float32,
        )
    names = lax.broadcasted_iota(jnp.int32, (owners, per_row), 0).astype(jnp.float32)
    named = (names == owner).astype(jnp.float32)
    earlier = (
        lax.broadcasted_iota(jnp.int32, (per_row, per_row), 0)
        < lax.broadcasted_iota(jnp.int32, (per_row, per_row), 1)
    ).astype(jnp.float32)
    rank = jnp.dot(named, earlier, preferred_element_type=jnp.float32)
    slot = jnp.sum(rank * named, axis=0, keepdims=True)
    spot = owner * capacity + slot
    rows = lax.broadcasted_iota(jnp.int32, (owners * capacity, per_row), 0).astype(jnp.float32)
    select[...] = (rows == spot).astype(jnp.float32)

    def turn_chunk(c, carry):
        w_copy(c).wait()
        for u in range(CHUNK // 2):
            for h in range(y_cells // 128):
                tall = jnp.concatenate(
                    [weights[c * CHUNK + 2 * u + i, :, h * 128 : (h + 1) * 128] for i in range(2)], axis=0
                ).T
                at = (c * (CHUNK // 2) + u) * y_cells
                for k in range(128 // runs):
                    turned[pl.ds(at + h * (128 // runs) + k, runs, stride=8), :] = tall[
                        k * runs : (k + 1) * runs
                    ]
        return carry

    lax.fori_loop(0, chunks, turn_chunk, 0)

    def ready():
        pl.semaphore_wait(barrier, slab + owners - 2)
        for d in range(1, slab):
            id_copy(d).start()

    def plan():
        for d in range(1, slab):
            id_copy(d).wait()
        lane = lax.broadcasted_iota(jnp.int32, (stations, per_row), 1) >> log2(keep)
        line = lane == lax.broadcasted_iota(jnp.int32, (stations, per_row), 0)
        flat = []
        for d in range(slab):
            ids = kept[0] if d == 0 else others[d - 1]
            wide = jnp.where(line, jnp.concatenate([ids] * stations, axis=1), 0)
            one = wide[0:1]
            for s in range(1, stations):
                one = one + wide[s : s + 1]
            flat.append(one)
        flat = jnp.concatenate(flat, axis=0)
        j = lax.broadcasted_iota(jnp.int32, (slab, per_row), 0)
        j = lax.rem(me - j + slab, slab)
        first, second, f0, f1, back = row_plan(flat, j, me, slab, half, x_cells, y_cells)
        rows_v[0] = first
        rows_v[1] = second
        row_copy().start()
        tall = jnp.concatenate([f0, f1, back, back], axis=0)
        tall = jnp.concatenate([tall, jnp.zeros((4 * slab, 128 - per_row), jnp.float32)], axis=1).T
        side = lax.broadcasted_iota(jnp.int32, (per_row, lanes), 1) < z_cells
        for d in range(slab):
            f0 = tall[:per_row, d : d + 1]
            f1 = tall[:per_row, slab + d : slab + d + 1]
            scale = jnp.where(side, f0, f1)
            for s in range(stations):
                z_part = kernel_scale * (zed[0:1] + height[s])
                scale_v[d, s * keep : (s + 1) * keep] = scale[s * keep : (s + 1) * keep] * z_part
            back_v[d] = jnp.broadcast_to(tall[:per_row, 2 * slab + d : 2 * slab + d + 1], (per_row, lanes))

    def station(s, carry):
        pl.when(s == 1)(ready)
        pl.when(s == stations - 1)(plan)
        east = (me * x_local).astype(jnp.float32) - place[0, s] * x_cells

        def where(row, v):
            if v == 0:
                return sums, (s * rows_x + row) * 8
            if v == 1:
                return halves, (s * rows_x + row) * 8
            return field, s * plane + row * y_cells + v * 8

        def put(row, v, value):
            ref, at = where(row, v)
            ref[pl.ds(pl.multiple_of(at, 8), 8), :] = value

        def get(row, v):
            ref, at = where(row, v)
            return ref[pl.ds(pl.multiple_of(at, 8), 8), :]

        for g in range(groups):
            easts = []
            for u in range(GROUP):
                e = beside + (east + float(2 * (g * GROUP + u)))
                easts.append(e * e)

            def emit(v, values):
                level, at = 0, g * GROUP
                while True:
                    for i, value in enumerate(values):
                        put(pyramid(pairs, level) + at + i, v, value)
                    if len(values) == 1:
                        break
                    values = [values[2 * i] + values[2 * i + 1] for i in range(len(values) // 2)]
                    level, at = level + 1, at // 2
                value = values[0]
                while at & 1:
                    value = get(pyramid(pairs, level) + at - 1, v) + value
                    level, at = level + 1, at // 2
                    put(pyramid(pairs, level) + at, v, value)

            stack = []
            for r in range(runs):
                t = table[s, r]
                values = []
                for u in range(GROUP):
                    inv = lax.rsqrt(t + easts[u])
                    w = turned[pl.ds(((g * GROUP + u) * runs + r) * 8, 8), :]
                    values.append((w * inv) * (inv * inv))
                level, run = 0, r
                while stack and stack[-1][0] == level:
                    _, other = stack.pop()
                    level, run = level + 1, run >> 1
                    emit((runs >> level) + run, [o - v for o, v in zip(other, values)])
                    values = [o + v for o, v in zip(other, values)]
                stack.append((level, values))
            emit(0, stack[0][1])
        return carry

    lax.fori_loop(0, stations, station, 0)

    def finish_y(tile, carry):
        at = pl.multiple_of(tile * 64, 64)
        values = tree([sums[pl.ds(at + i, 8, stride=8), :] for i in range(8)])
        values = values + [halves[pl.ds(at + i, 8, stride=8), :] for i in range(8)]
        for b in range(16):
            to = (tile * 8 + b // 2) * y_cells + (b % 2) * 8
            field[pl.ds(pl.multiple_of(to, 8), 8), :] = values[b]
        return carry

    lax.fori_loop(0, stations * rows_x // 8, finish_y, 0)

    turn_z = jnp.concatenate([z_matrix(z_cells, 0), z_matrix(z_cells, 1)], axis=0)
    row_copy().wait()

    def part(d):
        for s in range(stations):
            for i in range(keep):
                k = s * keep + i
                taken[2 * k : 2 * k + 2, :] = field[pl.ds(s * plane + rows_s[0, d, k], 2, stride=8), :]
                given[2 * k : 2 * k + 2, :] = field[pl.ds(s * plane + rows_s[1, d, k], 2, stride=8), :]
        back, scale = back_v[d], scale_v[d]
        sides = [
            (taken[pl.ds(t, per_row, stride=2), :] + back * given[pl.ds(t, per_row, stride=2), :]) * scale
            for t in range(2)
        ]
        return jnp.dot(
            jnp.concatenate(sides, axis=1), turn_z,
            precision=lax.Precision.HIGHEST, preferred_element_type=jnp.float32,
        )

    def send_part(d, carry):
        parts[d] = part(d)
        part_copy(d).start()
        return carry

    lax.fori_loop(1, slab, send_part, 0)
    total = part(0)
    for d in range(1, slab):
        part_copy(d).wait()
        total = total + arrived[d - 1]
    packed[...] = jnp.dot(
        select[...], total, precision=lax.Precision.HIGHEST, preferred_element_type=jnp.float32
    ).reshape(packed.shape)
    for d in range(1, owners):
        out_copy(d).start()
    own = pltpu.make_async_copy(packed.at[q], out.at[q], own_sem)
    own.start()
    own.wait()
    for d in range(1, owners):
        out_copy(d).wait()


def local(station_place, station_height, cell_weight, kept, dest):
    slab = lax.axis_size("slab")
    owners = lax.axis_size("sta")
    x_local, y_cells, z_cells = cell_weight.shape
    stations = station_place.shape[0]
    keep = kept.shape[2]
    lanes = 2 * z_cells
    per_row = stations * keep
    capacity = max(2, 3 * per_row // owners)
    sizes = (slab, owners, stations, keep, x_local, y_cells, z_cells, capacity)
    dma = pltpu.SemaphoreType.DMA
    out = pl.pallas_call(
        functools.partial(whole_kernel, sizes),
        out_shape=jax.ShapeDtypeStruct((owners, capacity, lanes), jnp.float32),
        in_specs=[
            pl.BlockSpec(memory_space=pltpu.SMEM),
            pl.BlockSpec(memory_space=pltpu.SMEM),
            pl.BlockSpec(memory_space=pl.ANY),
            pl.BlockSpec(memory_space=pltpu.VMEM),
            pl.BlockSpec(memory_space=pltpu.VMEM),
        ],
        out_specs=pl.BlockSpec(memory_space=pl.ANY),
        scratch_shapes=[
            pltpu.VMEM((stations * x_local * y_cells, lanes), jnp.float32),
            pltpu.VMEM((stations * x_local * 8, lanes), jnp.float32),
            pltpu.VMEM((stations * x_local * 8, lanes), jnp.float32),
            pltpu.VMEM((x_local, z_cells, y_cells), jnp.float32),
            pltpu.VMEM((x_local // 2 * y_cells, lanes), jnp.float32),
            pltpu.VMEM((stations, y_cells // 8, 8, lanes), jnp.float32),
            pltpu.VMEM((owners * capacity, per_row), jnp.float32),
            pltpu.VMEM((slab - 1, stations, keep), jnp.int32),
            pltpu.VMEM((2, slab, per_row), jnp.int32),
            pltpu.SMEM((2, slab, per_row), jnp.int32),
            pltpu.VMEM((slab, per_row, lanes), jnp.float32),
            pltpu.VMEM((slab, per_row, lanes), jnp.float32),
            pltpu.VMEM((2 * per_row, lanes), jnp.float32),
            pltpu.VMEM((2 * per_row, lanes), jnp.float32),
            pltpu.VMEM((slab, per_row, lanes), jnp.float32),
            pltpu.VMEM((slab - 1, per_row, lanes), jnp.float32),
            pltpu.VMEM((owners, capacity, lanes), jnp.float32),
            dma((x_local // CHUNK,)),
            dma,
            dma((slab - 1,)),
            dma((slab - 1,)),
            dma((slab - 1,)),
            dma((slab - 1,)),
            dma((owners - 1,)),
            dma((owners - 1,)),
            dma,
        ],
        compiler_params=pltpu.CompilerParams(
            collective_id=0, has_side_effects=True, vmem_limit_bytes=60 * 1024 * 1024
        ),
    )(
        jnp.transpose(station_place),
        station_height,
        jnp.transpose(cell_weight, (0, 2, 1)),
        kept,
        jnp.transpose(dest, (0, 1, 3, 2)).reshape(stations, 1, keep),
    )
    return out.reshape(1, 1, owners, capacity, lanes)


def solution(mesh):
    placed = (
        P("sta", None),
        P("sta"),
        P("slab", None, None),
        P("slab", "sta", None),
        P("slab", "sta", None, None),
    )
    return jax.shard_map(
        local,
        mesh=mesh,
        in_specs=placed,
        out_specs=P("slab", "sta", None, None, None),
        check_vma=False,
    )
```

```python
import functools

import jax
import jax.numpy as jnp
from jax import lax
from jax.experimental import pallas as pl
from jax.experimental.pallas import tpu as pltpu
from jax.sharding import PartitionSpec as P

kernel_scale = 32.0
MESH = pl.DeviceIdType.MESH


def log2(n):
    return n.bit_length() - 1


def pyramid(pairs, level):
    return 2 * pairs - (2 * pairs >> level)


def row_plan(ids, j, me, slab, half, x_cells, y_cells):
    ls = log2(slab)
    pairs = x_cells // slab // 2
    a = ids >> log2(half)
    pair = j * half + (ids & (half - 1))
    total = pyramid(pairs, log2(pairs))
    first = jnp.full(a.shape, total, jnp.int32)
    second = jnp.full(a.shape, total, jnp.int32)
    factor = jnp.full(a.shape, x_cells ** -0.5, jnp.float32)
    turn = jnp.full(a.shape, 1.0, jnp.float32)
    back = jnp.full(a.shape, 0.0, jnp.float32)
    m = 1
    while m < x_cells:
        e = log2(m)
        at = a >= m
        k = a - m
        norm = (m / x_cells) ** 0.5
        if m >= slab:
            sh = e - ls
            mine = (k >> sh) == me
            here = k & ((1 << sh) - 1)
            factor = jnp.where(at, jnp.where(mine, norm, 0.0), factor)
            width = x_cells // m
            if width == 2:
                first = jnp.where(at, here, first)
                second = jnp.where(at, here, second)
                turn = jnp.where(at, -1.0, turn)
                back = jnp.where(at, 0.0, back)
            else:
                off = pyramid(pairs, log2(width) - 2)
                first = jnp.where(at, off + 2 * here, first)
                second = jnp.where(at, off + 2 * here + 1, second)
                back = jnp.where(at, -1.0, back)
        else:
            sh = ls - e
            mine = k == (me >> sh)
            sign = norm * (1 - 2 * ((me >> (sh - 1)) & 1)).astype(jnp.float32)
            factor = jnp.where(at, jnp.where(mine, sign, 0.0), factor)
        m = m * 2
    ynorm = jnp.full(a.shape, y_cells ** -0.5, jnp.float32)
    m = 1
    while m < y_cells // 2:
        ynorm = jnp.where(pair >= m, (2 * m / y_cells) ** 0.5, ynorm)
        m = m * 2

    def address(row):
        at = ((row & ~7) + pair) * y_cells + (row & 7)
        m = 16
        while m < y_cells:
            k = 2 * pair - m
            wide = m // 8
            spot = 8 * (wide + (k & (wide - 1))) + (k >> log2(wide))
            at = jnp.where(k >= 0, row * y_cells + spot, at)
            m = m * 2
        return at

    factor = factor * ynorm
    return address(first), address(second), factor, factor * turn, back


def z_matrix(z_cells, t):
    z = lax.broadcasted_iota(jnp.int32, (2 * z_cells, 2 * z_cells), 0) & (z_cells - 1)
    lane = lax.broadcasted_iota(jnp.int32, (2 * z_cells, 2 * z_cells), 1)
    c = lane & (z_cells - 1)
    value = jnp.full(z.shape, z_cells ** -0.5, jnp.float32)
    m = 1
    while m < z_cells:
        w = log2(z_cells // m)
        k = c - m
        norm = (m / z_cells) ** 0.5
        hit = (z >> w) == k
        up = ((z >> (w - 1)) & 1) == 0
        value = jnp.where(c >= m, jnp.where(hit, jnp.where(up, norm, -norm), 0.0), value)
        m = m * 2
    return jnp.where((lane >> log2(z_cells)) == t, value, 0.0)


def tree(values):
    out = [None] * len(values)
    while len(values) > 1:
        half = len(values) // 2
        for k in range(half):
            out[half + k] = values[2 * k] - values[2 * k + 1]
        values = [values[2 * k] + values[2 * k + 1] for k in range(half)]
    out[0] = values[0]
    return out


GROUP = 4
CHUNK = 8


def whole_kernel(
    sizes, place, height, w_hbm, kept, dest, out,
    field, sums, halves, weights, turned, table, select, others, rows_v, rows_s, scale_v, back_v,
    taken, given, parts, arrived, packed,
    w_sem, row_sem, i_send, i_recv, s_send, s_recv, o_send, o_recv, own_sem,
):
    slab, owners, stations, keep, x_local, y_cells, z_cells, capacity = sizes
    lanes = 2 * z_cells
    pairs = x_local // 2
    rows_x = 2 * pairs
    groups = pairs // GROUP
    chunks = x_local // CHUNK
    x_cells = x_local * slab
    half = y_cells // slab // 2
    per_row = stations * keep
    runs = y_cells // 8
    me, q = lax.axis_index("slab"), lax.axis_index("sta")
    plane = rows_x * y_cells
    left = lax.broadcasted_iota(jnp.int32, (8, lanes), 1) < z_cells
    zed = (lax.broadcasted_iota(jnp.int32, (8, lanes), 1) & (z_cells - 1)).astype(jnp.float32) + 0.5
    beside = jnp.where(left, 0.5, 1.5)

    def before(d):
        return lax.rem(me - d + slab, slab)

    def id_copy(d):
        return pltpu.make_async_remote_copy(
            src_ref=kept.at[0],
            dst_ref=others.at[d - 1],
            send_sem=i_send.at[d - 1],
            recv_sem=i_recv.at[d - 1],
            device_id=(lax.rem(me + d, slab), q),
            device_id_type=MESH,
        )

    def part_copy(d):
        return pltpu.make_async_remote_copy(
            src_ref=parts.at[d],
            dst_ref=arrived.at[d - 1],
            send_sem=s_send.at[d - 1],
            recv_sem=s_recv.at[d - 1],
            device_id=(before(d), q),
            device_id_type=MESH,
        )

    def out_copy(d):
        to = lax.rem(q + d, owners)
        return pltpu.make_async_remote_copy(
            src_ref=packed.at[to],
            dst_ref=out.at[q],
            send_sem=o_send.at[d - 1],
            recv_sem=o_recv.at[d - 1],
            device_id=(me, to),
            device_id_type=MESH,
        )

    def row_copy():
        return pltpu.make_async_copy(rows_v, rows_s, row_sem)

    def w_copy(c):
        return pltpu.make_async_copy(
            w_hbm.at[pl.ds(c * CHUNK, CHUNK)], weights.at[pl.ds(c * CHUNK, CHUNK)], w_sem.at[c]
        )

    for c in range(chunks):
        w_copy(c).start()
    barrier = pltpu.get_barrier_semaphore()
    for d in range(1, slab):
        pl.semaphore_signal(
            barrier, inc=1, device_id=(lax.rem(me + d, slab), q), device_id_type=MESH
        )
    for d in range(1, owners):
        pl.semaphore_signal(
            barrier, inc=1, device_id=(me, lax.rem(q + d, owners)), device_id_type=MESH
        )

    base = (lax.broadcasted_iota(jnp.int32, (8, lanes), 0) * runs).astype(jnp.float32) + 0.5
    for s in range(stations):
        depth = zed + height[s]
        square = depth * depth
        north = base - place[1, s] * y_cells
        for r in range(runs):
            n = north + float(r)
            table[s, r] = n * n + square
    owner = jnp.zeros((1, per_row), jnp.float32)
    for s in range(stations):
        spread = lax.broadcasted_iota(jnp.int32, (keep, per_row), 1) == (
            lax.broadcasted_iota(jnp.int32, (keep, per_row), 0) + s * keep
        )
        owner = owner + jnp.dot(
            dest[s].astype(jnp.float32), spread.astype(jnp.float32),
            preferred_element_type=jnp.float32,
        )
    names = lax.broadcasted_iota(jnp.int32, (owners, per_row), 0).astype(jnp.float32)
    named = (names == owner).astype(jnp.float32)
    earlier = (
        lax.broadcasted_iota(jnp.int32, (per_row, per_row), 0)
        < lax.broadcasted_iota(jnp.int32, (per_row, per_row), 1)
    ).astype(jnp.float32)
    rank = jnp.dot(named, earlier, preferred_element_type=jnp.float32)
    slot = jnp.sum(rank * named, axis=0, keepdims=True)
    spot = owner * capacity + slot
    rows = lax.broadcasted_iota(jnp.int32, (owners * capacity, per_row), 0).astype(jnp.float32)
    select[...] = (rows == spot).astype(jnp.float32)

    def turn_chunk(c, carry):
        w_copy(c).wait()
        for u in range(CHUNK // 2):
            for h in range(y_cells // 128):
                tall = jnp.concatenate(
                    [weights[c * CHUNK + 2 * u + i, :, h * 128 : (h + 1) * 128] for i in range(2)], axis=0
                ).T
                at = (c * (CHUNK // 2) + u) * y_cells
                for k in range(128 // runs):
                    turned[pl.ds(at + h * (128 // runs) + k, runs, stride=8), :] = tall[
                        k * runs : (k + 1) * runs
                    ]
        return carry

    lax.fori_loop(0, chunks, turn_chunk, 0)

    def ready():
        pl.semaphore_wait(barrier, slab + owners - 2)
        for d in range(1, slab):
            id_copy(d).start()

    def plan():
        for d in range(1, slab):
            id_copy(d).wait()
        lane = lax.broadcasted_iota(jnp.int32, (stations, per_row), 1) >> log2(keep)
        line = lane == lax.broadcasted_iota(jnp.int32, (stations, per_row), 0)
        flat = []
        for d in range(slab):
            ids = kept[0] if d == 0 else others[d - 1]
            wide = jnp.where(line, jnp.concatenate([ids] * stations, axis=1), 0)
            one = wide[0:1]
            for s in range(1, stations):
                one = one + wide[s : s + 1]
            flat.append(one)
        flat = jnp.concatenate(flat, axis=0)
        j = lax.broadcasted_iota(jnp.int32, (slab, per_row), 0)
        j = lax.rem(me - j + slab, slab)
        first, second, f0, f1, back = row_plan(flat, j, me, slab, half, x_cells, y_cells)
        rows_v[0] = first
        rows_v[1] = second
        row_copy().start()
        tall = jnp.concatenate([f0, f1, back, back], axis=0)
        tall = jnp.concatenate([tall, jnp.zeros((4 * slab, 128 - per_row), jnp.float32)], axis=1).T
        side = lax.broadcasted_iota(jnp.int32, (per_row, lanes), 1) < z_cells
        for d in range(slab):
            f0 = tall[:per_row, d : d + 1]
            f1 = tall[:per_row, slab + d : slab + d + 1]
            scale = jnp.where(side, f0, f1)
            for s in range(stations):
                z_part = kernel_scale * (zed[0:1] + height[s])
                scale_v[d, s * keep : (s + 1) * keep] = scale[s * keep : (s + 1) * keep] * z_part
            back_v[d] = jnp.broadcast_to(tall[:per_row, 2 * slab + d : 2 * slab + d + 1], (per_row, lanes))

    def station(s, carry):
        pl.when(s == 1)(ready)
        pl.when(s == stations - 1)(plan)
        east = (me * x_local).astype(jnp.float32) - place[0, s] * x_cells

        def where(row, v):
            if v == 0:
                return sums, (s * rows_x + row) * 8
            if v == 1:
                return halves, (s * rows_x + row) * 8
            return field, s * plane + row * y_cells + v * 8

        def put(row, v, value):
            ref, at = where(row, v)
            ref[pl.ds(pl.multiple_of(at, 8), 8), :] = value

        def get(row, v):
            ref, at = where(row, v)
            return ref[pl.ds(pl.multiple_of(at, 8), 8), :]

        for g in range(groups):
            easts = []
            for u in range(GROUP):
                e = beside + (east + float(2 * (g * GROUP + u)))
                easts.append(e * e)

            def emit(v, values):
                level, at = 0, g * GROUP
                while True:
                    for i, value in enumerate(values):
                        put(pyramid(pairs, level) + at + i, v, value)
                    if len(values) == 1:
                        break
                    values = [values[2 * i] + values[2 * i + 1] for i in range(len(values) // 2)]
                    level, at = level + 1, at // 2
                value = values[0]
                while at & 1:
                    value = get(pyramid(pairs, level) + at - 1, v) + value
                    level, at = level + 1, at // 2
                    put(pyramid(pairs, level) + at, v, value)

            stack = []
            for r in range(runs):
                t = table[s, r]
                values = []
                for u in range(GROUP):
                    inv = lax.rsqrt(t + easts[u])
                    w = turned[pl.ds(((g * GROUP + u) * runs + r) * 8, 8), :]
                    values.append((w * inv) * (inv * inv))
                level, run = 0, r
                while stack and stack[-1][0] == level:
                    _, other = stack.pop()
                    level, run = level + 1, run >> 1
                    emit((runs >> level) + run, [o - v for o, v in zip(other, values)])
                    values = [o + v for o, v in zip(other, values)]
                stack.append((level, values))
            emit(0, stack[0][1])
        return carry

    lax.fori_loop(0, stations, station, 0)

    def finish_y(tile, carry):
        at = pl.multiple_of(tile * 64, 64)
        values = tree([sums[pl.ds(at + i, 8, stride=8), :] for i in range(8)])
        values = values + [halves[pl.ds(at + i, 8, stride=8), :] for i in range(8)]
        for b in range(16):
            to = (tile * 8 + b // 2) * y_cells + (b % 2) * 8
            field[pl.ds(pl.multiple_of(to, 8), 8), :] = values[b]
        return carry

    lax.fori_loop(0, stations * rows_x // 8, finish_y, 0)

    turn_z = jnp.concatenate([z_matrix(z_cells, 0), z_matrix(z_cells, 1)], axis=0)
    row_copy().wait()

    def part(d):
        for s in range(stations):
            for i in range(keep):
                k = s * keep + i
                taken[2 * k : 2 * k + 2, :] = field[pl.ds(s * plane + rows_s[0, d, k], 2, stride=8), :]
                given[2 * k : 2 * k + 2, :] = field[pl.ds(s * plane + rows_s[1, d, k], 2, stride=8), :]
        back, scale = back_v[d], scale_v[d]
        sides = [
            (taken[pl.ds(t, per_row, stride=2), :] + back * given[pl.ds(t, per_row, stride=2), :]) * scale
            for t in range(2)
        ]
        return jnp.dot(
            jnp.concatenate(sides, axis=1), turn_z,
            precision=lax.Precision.HIGHEST, preferred_element_type=jnp.float32,
        )

    def send_part(d, carry):
        parts[d] = part(d)
        part_copy(d).start()
        return carry

    lax.fori_loop(1, slab, send_part, 0)
    total = part(0)
    for d in range(1, slab):
        part_copy(d).wait()
        total = total + arrived[d - 1]
    packed[...] = jnp.dot(
        select[...], total, precision=lax.Precision.HIGHEST, preferred_element_type=jnp.float32
    ).reshape(packed.shape)
    for d in range(1, owners):
        out_copy(d).start()
    own = pltpu.make_async_copy(packed.at[q], out.at[q], own_sem)
    own.start()
    own.wait()
    for d in range(1, owners):
        out_copy(d).wait()


def local(station_place, station_height, cell_weight, kept, dest):
    slab = lax.axis_size("slab")
    owners = lax.axis_size("sta")
    x_local, y_cells, z_cells = cell_weight.shape
    stations = station_place.shape[0]
    keep = kept.shape[2]
    lanes = 2 * z_cells
    per_row = stations * keep
    capacity = max(2, 3 * per_row // owners)
    sizes = (slab, owners, stations, keep, x_local, y_cells, z_cells, capacity)
    dma = pltpu.SemaphoreType.DMA
    out = pl.pallas_call(
        functools.partial(whole_kernel, sizes),
        out_shape=pltpu.VMEM((owners, capacity, lanes), jnp.float32),
        in_specs=[
            pl.BlockSpec(memory_space=pltpu.SMEM),
            pl.BlockSpec(memory_space=pltpu.SMEM),
            pl.BlockSpec(memory_space=pl.ANY),
            pl.BlockSpec(memory_space=pltpu.VMEM),
            pl.BlockSpec(memory_space=pltpu.VMEM),
        ],
        out_specs=pl.BlockSpec(memory_space=pl.ANY),
        scratch_shapes=[
            pltpu.VMEM((stations * x_local * y_cells, lanes), jnp.float32),
            pltpu.VMEM((stations * x_local * 8, lanes), jnp.float32),
            pltpu.VMEM((stations * x_local * 8, lanes), jnp.float32),
            pltpu.VMEM((x_local, z_cells, y_cells), jnp.float32),
            pltpu.VMEM((x_local // 2 * y_cells, lanes), jnp.float32),
            pltpu.VMEM((stations, y_cells // 8, 8, lanes), jnp.float32),
            pltpu.VMEM((owners * capacity, per_row), jnp.float32),
            pltpu.VMEM((slab - 1, stations, keep), jnp.int32),
            pltpu.VMEM((2, slab, per_row), jnp.int32),
            pltpu.SMEM((2, slab, per_row), jnp.int32),
            pltpu.VMEM((slab, per_row, lanes), jnp.float32),
            pltpu.VMEM((slab, per_row, lanes), jnp.float32),
            pltpu.VMEM((2 * per_row, lanes), jnp.float32),
            pltpu.VMEM((2 * per_row, lanes), jnp.float32),
            pltpu.VMEM((slab, per_row, lanes), jnp.float32),
            pltpu.VMEM((slab - 1, per_row, lanes), jnp.float32),
            pltpu.VMEM((owners, capacity, lanes), jnp.float32),
            dma((x_local // CHUNK,)),
            dma,
            dma((slab - 1,)),
            dma((slab - 1,)),
            dma((slab - 1,)),
            dma((slab - 1,)),
            dma((owners - 1,)),
            dma((owners - 1,)),
            dma,
        ],
        compiler_params=pltpu.CompilerParams(
            collective_id=0, has_side_effects=True, vmem_limit_bytes=48_000_000
        ),
    )(
        *(
            pltpu.with_memory_space_constraint(a, pltpu.HBM)
            for a in (
                jnp.transpose(station_place),
                station_height,
                jnp.transpose(cell_weight, (0, 2, 1)),
                kept,
                jnp.transpose(dest, (0, 1, 3, 2)).reshape(stations, 1, keep),
            )
        )
    )
    return out.reshape(1, 1, owners, capacity, lanes)


def solution(mesh):
    placed = (
        P("sta", None),
        P("sta"),
        P("slab", None, None),
        P("slab", "sta", None),
        P("slab", "sta", None, None),
    )
    return jax.shard_map(
        local,
        mesh=mesh,
        in_specs=placed,
        out_specs=P("slab", "sta", None, None, None),
        check_vma=False,
    )
```

```python
import functools

import jax
import jax.numpy as jnp
from jax import lax
from jax.experimental import pallas as pl
from jax.experimental.pallas import tpu as pltpu
from jax.sharding import PartitionSpec as P

kernel_scale = 32.0
MESH = pl.DeviceIdType.MESH


def log2(n):
    return n.bit_length() - 1


def pyramid(pairs, level):
    return 2 * pairs - (2 * pairs >> level)


def row_plan(ids, j, me, slab, half, x_cells, y_cells):
    ls = log2(slab)
    pairs = x_cells // slab // 2
    a = ids >> log2(half)
    pair = j * half + (ids & (half - 1))
    total = pyramid(pairs, log2(pairs))
    first = jnp.full(a.shape, total, jnp.int32)
    second = jnp.full(a.shape, total, jnp.int32)
    factor = jnp.full(a.shape, x_cells ** -0.5, jnp.float32)
    turn = jnp.full(a.shape, 1.0, jnp.float32)
    back = jnp.full(a.shape, 0.0, jnp.float32)
    m = 1
    while m < x_cells:
        e = log2(m)
        at = a >= m
        k = a - m
        norm = (m / x_cells) ** 0.5
        if m >= slab:
            sh = e - ls
            mine = (k >> sh) == me
            here = k & ((1 << sh) - 1)
            factor = jnp.where(at, jnp.where(mine, norm, 0.0), factor)
            width = x_cells // m
            if width == 2:
                first = jnp.where(at, here, first)
                second = jnp.where(at, here, second)
                turn = jnp.where(at, -1.0, turn)
                back = jnp.where(at, 0.0, back)
            else:
                off = pyramid(pairs, log2(width) - 2)
                first = jnp.where(at, off + 2 * here, first)
                second = jnp.where(at, off + 2 * here + 1, second)
                back = jnp.where(at, -1.0, back)
        else:
            sh = ls - e
            mine = k == (me >> sh)
            sign = norm * (1 - 2 * ((me >> (sh - 1)) & 1)).astype(jnp.float32)
            factor = jnp.where(at, jnp.where(mine, sign, 0.0), factor)
        m = m * 2
    ynorm = jnp.full(a.shape, y_cells ** -0.5, jnp.float32)
    m = 1
    while m < y_cells // 2:
        ynorm = jnp.where(pair >= m, (2 * m / y_cells) ** 0.5, ynorm)
        m = m * 2

    def address(row):
        at = ((row & ~7) + pair) * y_cells + (row & 7)
        m = 16
        while m < y_cells:
            k = 2 * pair - m
            wide = m // 8
            spot = 8 * (wide + (k & (wide - 1))) + (k >> log2(wide))
            at = jnp.where(k >= 0, row * y_cells + spot, at)
            m = m * 2
        return at

    factor = factor * ynorm
    return address(first), address(second), factor, factor * turn, back


def z_signs(z_cells, t):
    z = lax.broadcasted_iota(jnp.int32, (2 * z_cells, 2 * z_cells), 0) & (z_cells - 1)
    lane = lax.broadcasted_iota(jnp.int32, (2 * z_cells, 2 * z_cells), 1)
    c = lane & (z_cells - 1)
    value = jnp.full(z.shape, 1.0, jnp.float32)
    m = 1
    while m < z_cells:
        w = log2(z_cells // m)
        k = c - m
        hit = (z >> w) == k
        up = ((z >> (w - 1)) & 1) == 0
        value = jnp.where(c >= m, jnp.where(hit, jnp.where(up, 1.0, -1.0), 0.0), value)
        m = m * 2
    return jnp.where((lane >> log2(z_cells)) == t, value, 0.0)


def z_norms(z_cells):
    c = lax.broadcasted_iota(jnp.int32, (8, 2 * z_cells), 1) & (z_cells - 1)
    norm = jnp.full(c.shape, z_cells ** -0.5, jnp.float32)
    m = 1
    while m < z_cells:
        norm = jnp.where(c >= m, (m / z_cells) ** 0.5, norm)
        m = m * 2
    return norm


def pieces(x):
    high = x.astype(jnp.bfloat16)
    rest = x - high.astype(jnp.float32)
    middle = rest.astype(jnp.bfloat16)
    low = (rest - middle.astype(jnp.float32)).astype(jnp.bfloat16)
    return jnp.concatenate([high, middle, low], axis=0)


def tree(values):
    out = [None] * len(values)
    while len(values) > 1:
        half = len(values) // 2
        for k in range(half):
            out[half + k] = values[2 * k] - values[2 * k + 1]
        values = [values[2 * k] + values[2 * k + 1] for k in range(half)]
    out[0] = values[0]
    return out


GROUP = 4
CHUNK = 2 * GROUP


def whole_kernel(
    sizes, place_h, height_h, w_hbm, kept_h, dest_h, out,
    fields, sums, halves, place, height, kept, dest,
    weights, turned, table, select, signs, others, rows_v, rows_s, scale_v, back_v,
    taken, given, parts, arrived, packed,
    w_sem, in_sem, row_sem, i_send, i_recv, s_send, s_recv, o_send, o_recv, own_sem,
):
    slab, owners, stations, keep, x_local, y_cells, z_cells, capacity = sizes
    lanes = 2 * z_cells
    pairs = x_local // 2
    rows_x = 2 * pairs
    groups = pairs // GROUP
    x_cells = x_local * slab
    half = y_cells // slab // 2
    per_row = stations * keep
    runs = y_cells // 8
    me, q = lax.axis_index("slab"), lax.axis_index("sta")
    zed = (lax.broadcasted_iota(jnp.int32, (8, lanes), 1) & (z_cells - 1)).astype(jnp.float32) + 0.5

    def before(d):
        return lax.rem(me - d + slab, slab)

    def id_copy(d):
        return pltpu.make_async_remote_copy(
            src_ref=kept,
            dst_ref=others.at[d - 1],
            send_sem=i_send.at[d - 1],
            recv_sem=i_recv.at[d - 1],
            device_id=(lax.rem(me + d, slab), q),
            device_id_type=MESH,
        )

    def part_copy(s, d):
        return pltpu.make_async_remote_copy(
            src_ref=parts.at[s, d],
            dst_ref=arrived.at[s, d - 1],
            send_sem=s_send.at[s, d - 1],
            recv_sem=s_recv.at[s, d - 1],
            device_id=(before(d), q),
            device_id_type=MESH,
        )

    def out_copy(d):
        to = lax.rem(q + d, owners)
        return pltpu.make_async_remote_copy(
            src_ref=packed.at[to],
            dst_ref=out.at[q],
            send_sem=o_send.at[d - 1],
            recv_sem=o_recv.at[d - 1],
            device_id=(me, to),
            device_id_type=MESH,
        )

    def row_copy():
        return pltpu.make_async_copy(rows_v, rows_s, row_sem)

    def w_copy(c):
        return pltpu.make_async_copy(
            w_hbm.at[pl.ds(c * CHUNK, CHUNK)], weights.at[pl.ds(c * CHUNK, CHUNK)], w_sem.at[c]
        )

    inputs = [
        pltpu.make_async_copy(a, b, in_sem.at[i])
        for i, (a, b) in enumerate(
            [(place_h, place), (height_h, height), (kept_h.at[0], kept), (dest_h, dest)]
        )
    ]
    for copy in inputs:
        copy.start()
    for c in range(groups):
        w_copy(c).start()
    barrier = pltpu.get_barrier_semaphore()
    for d in range(1, slab):
        pl.semaphore_signal(
            barrier, inc=1, device_id=(lax.rem(me + d, slab), q), device_id_type=MESH
        )
    for d in range(1, owners):
        pl.semaphore_signal(
            barrier, inc=1, device_id=(me, lax.rem(q + d, owners)), device_id_type=MESH
        )
    signs[...] = jnp.concatenate([z_signs(z_cells, 0), z_signs(z_cells, 1)], axis=0).astype(jnp.bfloat16)
    for copy in inputs:
        copy.wait()

    def heights(s):
        base = (lax.broadcasted_iota(jnp.int32, (8, lanes), 0) * runs).astype(jnp.float32) + 0.5
        depth = zed + height[s]
        square = depth * depth
        north = base - place[1, s] * y_cells
        for r in range(runs):
            n = north + float(r)
            table[s, r] = n * n + square

    def choose():
        owner = jnp.zeros((1, per_row), jnp.float32)
        for s in range(stations):
            spread = lax.broadcasted_iota(jnp.int32, (keep, per_row), 1) == (
                lax.broadcasted_iota(jnp.int32, (keep, per_row), 0) + s * keep
            )
            owner = owner + jnp.dot(
                dest[s].astype(jnp.float32), spread.astype(jnp.float32),
                preferred_element_type=jnp.float32,
            )
        names = lax.broadcasted_iota(jnp.int32, (owners, per_row), 0).astype(jnp.float32)
        named = (names == owner).astype(jnp.float32)
        earlier = (
            lax.broadcasted_iota(jnp.int32, (per_row, per_row), 0)
            < lax.broadcasted_iota(jnp.int32, (per_row, per_row), 1)
        ).astype(jnp.float32)
        rank = jnp.dot(named, earlier, preferred_element_type=jnp.float32)
        slot = jnp.sum(rank * named, axis=0, keepdims=True)
        spot = owner * capacity + slot
        rows = lax.broadcasted_iota(jnp.int32, (owners * capacity, per_row), 0).astype(jnp.float32)
        chosen = (rows == spot).astype(jnp.float32)
        cut = (stations - 1) * keep
        wide = jnp.concatenate([chosen[:, :cut]] * 3 + [chosen[:, cut:]] * 3, axis=1)
        select[...] = wide.astype(jnp.bfloat16)

    def push(c, u, h):
        return jnp.concatenate(
            [weights[c * CHUNK + 2 * u + i, :, h * 128 : (h + 1) * 128] for i in range(2)], axis=0
        ).T

    def drop(c, u, h, tall):
        for k in range(128 // runs):
            turned[c * GROUP + u, pl.ds(h * (128 // runs) + k, runs, stride=8), :] = tall[
                k * runs : (k + 1) * runs
            ]

    tiles = [(u, h) for u in range(GROUP) for h in range(y_cells // 128)]

    def ready():
        pl.semaphore_wait(barrier, slab + owners - 2)
        for d in range(1, slab):
            id_copy(d).start()

    held = {}

    def plan_ids():
        for d in range(1, slab):
            id_copy(d).wait()

    def plan_rows():
        lane = lax.broadcasted_iota(jnp.int32, (stations, per_row), 1) >> log2(keep)
        line = lane == lax.broadcasted_iota(jnp.int32, (stations, per_row), 0)
        flat = []
        for d in range(slab):
            ids = kept[...] if d == 0 else others[d - 1]
            wide = jnp.where(line, jnp.concatenate([ids] * stations, axis=1), 0)
            one = wide[0:1]
            for s in range(1, stations):
                one = one + wide[s : s + 1]
            flat.append(one)
        flat = jnp.concatenate(flat, axis=0)
        j = lax.broadcasted_iota(jnp.int32, (slab, per_row), 0)
        j = lax.rem(me - j + slab, slab)
        first, second, f0, f1, back = row_plan(flat, j, me, slab, half, x_cells, y_cells)
        rows_v[0] = first
        rows_v[1] = second
        tall = jnp.concatenate([f0, f1, back, back], axis=0)
        tall = jnp.concatenate([tall, jnp.zeros((4 * slab, 128 - per_row), jnp.float32)], axis=1)
        held["tall"] = tall.T

    def plan_scale(s, d):
        tall = held["tall"]
        side = lax.broadcasted_iota(jnp.int32, (keep, lanes), 1) < z_cells
        z_part = kernel_scale * (zed[0:1] + height[s])
        k = s * keep
        f0 = tall[k : k + keep, d : d + 1]
        f1 = tall[k : k + keep, slab + d : slab + d + 1]
        back = tall[k : k + keep, 2 * slab + d : 2 * slab + d + 1]
        scale_v[s, d * keep : (d + 1) * keep] = jnp.where(side, f0, f1) * z_part
        back_v[s, d * keep : (d + 1) * keep] = jnp.broadcast_to(back, (keep, lanes))

    def finish_y(s, tile):
        at = (s * rows_x + tile * 8) * 8
        values = tree([sums[pl.ds(at + i, 8, stride=8), :] for i in range(8)])
        values = values + [halves[pl.ds(at + i, 8, stride=8), :] for i in range(8)]
        for b in range(16):
            to = (tile * 8 + b // 2) * y_cells + (b % 2) * 8
            fields[s][pl.ds(to, 8), :] = values[b]

    def last_group(row):
        level = 0
        while row >= pyramid(pairs, level + 1):
            level = level + 1
        return min(pairs - 1, ((row - pyramid(pairs, level) + 1) << level) - 1) // GROUP

    def finished(g):
        ready_at = [max(last_group(8 * t + i) for i in range(8)) for t in range(rows_x // 8)]
        return [t for t, at in enumerate(ready_at) if at == g]

    def gather(s, k):
        d, i = k // keep, k % keep
        for n in range(2):
            to = taken if n == 0 else given
            to[s, 2 * k : 2 * k + 2, :] = fields[s][pl.ds(rows_s[n, d, s * keep + i], 2, stride=8), :]

    blocks = slab * keep

    def depth_dot(s):
        back, scale = back_v[s], scale_v[s]
        sides = []
        for t in range(2):
            mine = pl.ds(t, blocks, stride=2)
            sides.append((taken[s, mine, :] + back * given[s, mine, :]) * scale)
        held[s] = jnp.dot(
            pieces(jnp.concatenate(sides, axis=1)), signs[...], preferred_element_type=jnp.float32
        )

    def send(s):
        tall = held.pop(s)
        rows = (tall[2 * blocks :] + tall[blocks : 2 * blocks]) + tall[:blocks]
        rows = rows * z_norms(z_cells)[0:1]
        for d in range(slab):
            parts[s, d] = rows[d * keep : (d + 1) * keep]
        for d in range(1, slab):
            part_copy(s, d).start()

    def total(s):
        value = parts[s, 0]
        for d in range(1, slab):
            part_copy(s, d).wait()
            value = value + arrived[s, d - 1]
        return value

    far = 2 * lax.broadcasted_iota(jnp.int32, (GROUP, 8, lanes), 0)
    far = far.astype(jnp.float32) + jnp.where(
        lax.broadcasted_iota(jnp.int32, (GROUP, 8, lanes), 2) < z_cells, 0.5, 1.5
    )

    def evaluate(s, g, before_run):
        east = (me * x_local).astype(jnp.float32) - place[0, s] * x_cells

        def where(row, v):
            if v == 0:
                return sums, (s * rows_x + row) * 8
            if v == 1:
                return halves, (s * rows_x + row) * 8
            return fields[s], row * y_cells + v * 8

        def put(row, v, value):
            ref, at = where(row, v)
            ref[pl.ds(at, 8), :] = value

        def get(row, v):
            ref, at = where(row, v)
            return ref[pl.ds(at, 8), :]

        e = far + (east + float(2 * g * GROUP))
        easts = e * e

        def emit(v, wide):
            values = [wide[i] for i in range(GROUP)]
            level, at = 0, g * GROUP
            while True:
                for i, value in enumerate(values):
                    put(pyramid(pairs, level) + at + i, v, value)
                if len(values) == 1:
                    break
                values = [values[2 * i] + values[2 * i + 1] for i in range(len(values) // 2)]
                level, at = level + 1, at // 2
            value = values[0]
            while at & 1:
                value = get(pyramid(pairs, level) + at - 1, v) + value
                level, at = level + 1, at // 2
                put(pyramid(pairs, level) + at, v, value)

        stack = []
        for r in range(runs):
            before_run(r)
            inv = lax.rsqrt(table[s, r] + easts)
            w = turned[g * GROUP : (g + 1) * GROUP, r * 8 : r * 8 + 8, :]
            values = (w * inv) * (inv * inv)
            level, run = 0, r
            while stack and stack[-1][0] == level:
                _, other = stack.pop()
                level, run = level + 1, run >> 1
                emit((runs >> level) + run, other - values)
                values = other + values
            stack.append((level, values))
        emit(0, stack[0][1])

    class Phase:
        def __init__(self, order):
            self.order, self.steps, self.work = order, len(order) * runs, {}

        def at(self, step, f, *args):
            step = min(int(step), self.steps - 1)
            self.work.setdefault(step, []).append(functools.partial(f, *args))

        def over(self, items, start, stop):
            for n, item in enumerate(items):
                self.at((start + (stop - start) * n / len(items)) * self.steps, *item)

        def tiles(self):
            for i, (s, g) in enumerate(self.order):
                if g < groups - 1:
                    for n, t in enumerate(finished(g)):
                        self.at((i + 1) * runs + 2 + 8 * n, finish_y, s, t)

        def run(self):
            for s in sorted({s for s, _ in self.order}):
                heights(s)
            for i, (s, g) in enumerate(self.order):
                def before_run(r, i=i):
                    for f in self.work.get(i * runs + r, ()):
                        f()
                evaluate(s, g, before_run)

    def tiles_after(s):
        return [(finish_y, s, t) for t in finished(groups - 1)]

    def gathers(s):
        return [(gather, s, k) for k in range(blocks)]

    def push_later(c, u, h):
        held[c, u, h] = push(c, u, h)

    def drop_later(c, u, h):
        drop(c, u, h, held.pop((c, u, h)))

    w_copy(0).wait()
    for u, h in tiles:
        drop(0, u, h, push(0, u, h))

    first = Phase([(s, g) for g in range(groups) for s in range(2)])
    for g in range(groups - 1):
        start = 2 * g * runs
        first.at(start, lambda c: w_copy(c).wait(), g + 1)
        for n, (u, h) in enumerate(tiles):
            first.at(start + 5 * n, push_later, g + 1, u, h)
            first.at(start + 5 * n + 18, drop_later, g + 1, u, h)
    first.at(2 * runs, ready)
    first.at(first.steps // 2, choose)
    first.tiles()
    first.run()

    second = Phase([(2, g) for g in range(groups)])
    second.over(tiles_after(0) + tiles_after(1), 0.0, 0.18)
    second.at(0.20 * second.steps, plan_ids)
    second.at(0.20 * second.steps, plan_rows)
    second.at(0.52 * second.steps, lambda: row_copy().start())
    second.over([(plan_scale, s, d) for s in range(stations) for d in range(slab)], 0.52, 0.70)
    second.at(0.70 * second.steps, lambda: row_copy().wait())
    second.over(gathers(0), 0.71, 0.99)
    second.tiles()
    second.run()

    third = Phase([(s, g) for s in range(3, stations) for g in range(groups)])
    third.over(tiles_after(2), 0.0, 0.1)
    third.at(0, depth_dot, 0)
    third.over(gathers(1), 0.02, 0.30)
    third.at(0.24 * third.steps, send, 0)
    third.at(0.31 * third.steps, depth_dot, 1)
    third.over(gathers(2), 0.33, 0.62)
    third.at(0.58 * third.steps, send, 1)
    third.at(0.64 * third.steps, depth_dot, 2)
    third.at(0.88 * third.steps, send, 2)
    third.tiles()
    third.run()

    for f, *args in tiles_after(3) + gathers(3):
        f(*args)
    depth_dot(3)
    send(3)
    most = jnp.concatenate([total(s) for s in range(stations - 1)], axis=0)
    cut = 3 * (stations - 1) * keep
    early = jnp.dot(select[:, :cut], pieces(most), preferred_element_type=jnp.float32)
    late = jnp.dot(
        select[:, cut:], pieces(total(stations - 1)), preferred_element_type=jnp.float32
    )
    packed[...] = (early + late).reshape(packed.shape)
    for d in range(1, owners):
        out_copy(d).start()
    own = pltpu.make_async_copy(packed.at[q], out.at[q], own_sem)
    own.start()
    own.wait()
    for d in range(1, owners):
        out_copy(d).wait()


def local(station_place, station_height, cell_weight, kept, dest):
    slab = lax.axis_size("slab")
    owners = lax.axis_size("sta")
    x_local, y_cells, z_cells = cell_weight.shape
    stations = station_place.shape[0]
    keep = kept.shape[2]
    lanes = 2 * z_cells
    per_row = stations * keep
    capacity = max(2, 3 * per_row // owners)
    sizes = (slab, owners, stations, keep, x_local, y_cells, z_cells, capacity)
    dma = pltpu.SemaphoreType.DMA
    f32, i32 = jnp.float32, jnp.int32
    out = pl.pallas_call(
        functools.partial(whole_kernel, sizes),
        out_shape=pltpu.VMEM((owners, capacity, lanes), f32),
        in_specs=[pl.BlockSpec(memory_space=pl.ANY)] * 5,
        out_specs=pl.BlockSpec(memory_space=pl.ANY),
        scratch_shapes=[
            [pltpu.VMEM((x_local * y_cells, lanes), f32)] * stations,
            pltpu.VMEM((stations * x_local * 8, lanes), f32),
            pltpu.VMEM((stations * x_local * 8, lanes), f32),
            pltpu.SMEM((2, stations), f32),
            pltpu.SMEM((stations,), f32),
            pltpu.VMEM((stations, keep), i32),
            pltpu.VMEM((stations, 1, keep), i32),
            pltpu.VMEM((x_local, z_cells, y_cells), f32),
            pltpu.VMEM((x_local // 2, y_cells, lanes), f32),
            pltpu.VMEM((stations, y_cells // 8, 8, lanes), f32),
            pltpu.VMEM((owners * capacity, 3 * per_row), jnp.bfloat16),
            pltpu.VMEM((2 * lanes, lanes), jnp.bfloat16),
            pltpu.VMEM((slab - 1, stations, keep), i32),
            pltpu.VMEM((2, slab, per_row), i32),
            pltpu.SMEM((2, slab, per_row), i32),
            pltpu.VMEM((stations, slab * keep, lanes), f32),
            pltpu.VMEM((stations, slab * keep, lanes), f32),
            pltpu.VMEM((stations, 2 * slab * keep, lanes), f32),
            pltpu.VMEM((stations, 2 * slab * keep, lanes), f32),
            pltpu.VMEM((stations, slab, keep, lanes), f32),
            pltpu.VMEM((stations, slab - 1, keep, lanes), f32),
            pltpu.VMEM((owners, capacity, lanes), f32),
            dma((x_local // CHUNK,)),
            dma((4,)),
            dma,
            dma((slab - 1,)),
            dma((slab - 1,)),
            dma((stations, slab - 1)),
            dma((stations, slab - 1)),
            dma((owners - 1,)),
            dma((owners - 1,)),
            dma,
        ],
        compiler_params=pltpu.CompilerParams(
            collective_id=0, has_side_effects=True, vmem_limit_bytes=52_000_000
        ),
    )(
        *(
            pltpu.with_memory_space_constraint(a, pltpu.HBM)
            for a in (
                jnp.transpose(station_place),
                station_height,
                jnp.transpose(cell_weight, (0, 2, 1)),
                kept,
                jnp.transpose(dest, (0, 1, 3, 2)).reshape(stations, 1, keep),
            )
        )
    )
    return out.reshape(1, 1, owners, capacity, lanes)


def solution(mesh):
    placed = (
        P("sta", None),
        P("sta"),
        P("slab", None, None),
        P("slab", "sta", None),
        P("slab", "sta", None, None),
    )
    return jax.shard_map(
        local,
        mesh=mesh,
        in_specs=placed,
        out_specs=P("slab", "sta", None, None, None),
        check_vma=False,
    )
```

```python
import functools

import jax
import jax.numpy as jnp
from jax import lax
from jax.experimental import pallas as pl
from jax.experimental.pallas import tpu as pltpu
from jax.sharding import PartitionSpec as P

kernel_scale = 32.0
MESH = pl.DeviceIdType.MESH


def log2(n):
    return n.bit_length() - 1


def pyramid(pairs, level):
    return 2 * pairs - (2 * pairs >> level)


def row_plan(ids, j, me, slab, half, x_cells, y_cells):
    ls = log2(slab)
    pairs = x_cells // slab // 2
    a = ids >> log2(half)
    pair = j * half + (ids & (half - 1))
    total = pyramid(pairs, log2(pairs))
    first = jnp.full(a.shape, total, jnp.int32)
    second = jnp.full(a.shape, total, jnp.int32)
    factor = jnp.full(a.shape, x_cells ** -0.5, jnp.float32)
    turn = jnp.full(a.shape, 1.0, jnp.float32)
    back = jnp.full(a.shape, 0.0, jnp.float32)
    m = 1
    while m < x_cells:
        e = log2(m)
        at = a >= m
        k = a - m
        norm = (m / x_cells) ** 0.5
        if m >= slab:
            sh = e - ls
            mine = (k >> sh) == me
            here = k & ((1 << sh) - 1)
            factor = jnp.where(at, jnp.where(mine, norm, 0.0), factor)
            width = x_cells // m
            if width == 2:
                first = jnp.where(at, here, first)
                second = jnp.where(at, here, second)
                turn = jnp.where(at, -1.0, turn)
                back = jnp.where(at, 0.0, back)
            else:
                off = pyramid(pairs, log2(width) - 2)
                first = jnp.where(at, off + 2 * here, first)
                second = jnp.where(at, off + 2 * here + 1, second)
                back = jnp.where(at, -1.0, back)
        else:
            sh = ls - e
            mine = k == (me >> sh)
            sign = norm * (1 - 2 * ((me >> (sh - 1)) & 1)).astype(jnp.float32)
            factor = jnp.where(at, jnp.where(mine, sign, 0.0), factor)
        m = m * 2
    ynorm = jnp.full(a.shape, y_cells ** -0.5, jnp.float32)
    m = 1
    while m < y_cells // 2:
        ynorm = jnp.where(pair >= m, (2 * m / y_cells) ** 0.5, ynorm)
        m = m * 2

    def address(row):
        at = ((row & ~7) + pair) * y_cells + (row & 7)
        m = 16
        while m < y_cells:
            k = 2 * pair - m
            wide = m // 8
            spot = 8 * (wide + (k & (wide - 1))) + (k >> log2(wide))
            at = jnp.where(k >= 0, row * y_cells + spot, at)
            m = m * 2
        return at

    factor = factor * ynorm
    return address(first), address(second), factor, factor * turn, back


def z_signs(z_cells, t):
    z = lax.broadcasted_iota(jnp.int32, (2 * z_cells, 2 * z_cells), 0) & (z_cells - 1)
    lane = lax.broadcasted_iota(jnp.int32, (2 * z_cells, 2 * z_cells), 1)
    c = lane & (z_cells - 1)
    value = jnp.full(z.shape, 1.0, jnp.float32)
    m = 1
    while m < z_cells:
        w = log2(z_cells // m)
        k = c - m
        hit = (z >> w) == k
        up = ((z >> (w - 1)) & 1) == 0
        value = jnp.where(c >= m, jnp.where(hit, jnp.where(up, 1.0, -1.0), 0.0), value)
        m = m * 2
    return jnp.where((lane >> log2(z_cells)) == t, value, 0.0)


def z_norms(z_cells):
    c = lax.broadcasted_iota(jnp.int32, (8, 2 * z_cells), 1) & (z_cells - 1)
    norm = jnp.full(c.shape, z_cells ** -0.5, jnp.float32)
    m = 1
    while m < z_cells:
        norm = jnp.where(c >= m, (m / z_cells) ** 0.5, norm)
        m = m * 2
    return norm


def pieces(x):
    high = x.astype(jnp.bfloat16)
    rest = x - high.astype(jnp.float32)
    middle = rest.astype(jnp.bfloat16)
    low = (rest - middle.astype(jnp.float32)).astype(jnp.bfloat16)
    return jnp.concatenate([high, middle, low], axis=0)


def tree(values):
    out = [None] * len(values)
    while len(values) > 1:
        half = len(values) // 2
        for k in range(half):
            out[half + k] = values[2 * k] - values[2 * k + 1]
        values = [values[2 * k] + values[2 * k + 1] for k in range(half)]
    out[0] = values[0]
    return out


GROUP = 4
CHUNK = 2 * GROUP


def whole_kernel(
    sizes, place_h, height_h, w_hbm, kept_h, dest_h, out,
    fields, sums, halves, place, height, kept, dest,
    weights, turned, table, select, signs, others, rows_v, rows_s, scale_v, back_v,
    taken, given, parts, arrived, packed,
    w_sem, in_sem, row_sem, i_send, i_recv, s_send, s_recv, o_send, o_recv, own_sem,
):
    slab, owners, stations, keep, x_local, y_cells, z_cells, capacity = sizes
    lanes = 2 * z_cells
    pairs = x_local // 2
    rows_x = 2 * pairs
    groups = pairs // GROUP
    x_cells = x_local * slab
    half = y_cells // slab // 2
    per_row = stations * keep
    runs = y_cells // 8
    me, q = lax.axis_index("slab"), lax.axis_index("sta")
    zed = (lax.broadcasted_iota(jnp.int32, (8, lanes), 1) & (z_cells - 1)).astype(jnp.float32) + 0.5

    def before(d):
        return lax.rem(me - d + slab, slab)

    def id_copy(d):
        return pltpu.make_async_remote_copy(
            src_ref=kept,
            dst_ref=others.at[d - 1],
            send_sem=i_send.at[d - 1],
            recv_sem=i_recv.at[d - 1],
            device_id=(lax.rem(me + d, slab), q),
            device_id_type=MESH,
        )

    def part_copy(s, d):
        return pltpu.make_async_remote_copy(
            src_ref=parts.at[s, d],
            dst_ref=arrived.at[s, d - 1],
            send_sem=s_send.at[s, d - 1],
            recv_sem=s_recv.at[s, d - 1],
            device_id=(before(d), q),
            device_id_type=MESH,
        )

    def out_copy(d):
        to = lax.rem(q + d, owners)
        return pltpu.make_async_remote_copy(
            src_ref=packed.at[to],
            dst_ref=out.at[q],
            send_sem=o_send.at[d - 1],
            recv_sem=o_recv.at[d - 1],
            device_id=(me, to),
            device_id_type=MESH,
        )

    def row_copy():
        return pltpu.make_async_copy(rows_v, rows_s, row_sem)

    def w_copy(c):
        return pltpu.make_async_copy(
            w_hbm.at[pl.ds(c * CHUNK, CHUNK)], weights.at[pl.ds(c * CHUNK, CHUNK)], w_sem.at[c]
        )

    inputs = [
        pltpu.make_async_copy(a, b, in_sem.at[i])
        for i, (a, b) in enumerate(
            [(place_h, place), (height_h, height), (kept_h.at[0], kept), (dest_h, dest)]
        )
    ]
    for copy in inputs:
        copy.start()
    for c in range(groups):
        w_copy(c).start()
    barrier = pltpu.get_barrier_semaphore()
    for d in range(1, slab):
        pl.semaphore_signal(
            barrier, inc=1, device_id=(lax.rem(me + d, slab), q), device_id_type=MESH
        )
    for d in range(1, owners):
        pl.semaphore_signal(
            barrier, inc=1, device_id=(me, lax.rem(q + d, owners)), device_id_type=MESH
        )
    signs[...] = jnp.concatenate([z_signs(z_cells, 0), z_signs(z_cells, 1)], axis=0).astype(jnp.bfloat16)
    for copy in inputs:
        copy.wait()

    def heights(s):
        base = (lax.broadcasted_iota(jnp.int32, (8, lanes), 0) * runs).astype(jnp.float32) + 0.5
        depth = zed + height[s]
        square = depth * depth
        north = base - place[1, s] * y_cells
        for r in range(runs):
            n = north + float(r)
            table[s, r] = n * n + square

    def choose():
        owner = jnp.zeros((1, per_row), jnp.float32)
        for s in range(stations):
            spread = lax.broadcasted_iota(jnp.int32, (keep, per_row), 1) == (
                lax.broadcasted_iota(jnp.int32, (keep, per_row), 0) + s * keep
            )
            owner = owner + jnp.dot(
                dest[s].astype(jnp.float32), spread.astype(jnp.float32),
                preferred_element_type=jnp.float32,
            )
        names = lax.broadcasted_iota(jnp.int32, (owners, per_row), 0).astype(jnp.float32)
        named = (names == owner).astype(jnp.float32)
        earlier = (
            lax.broadcasted_iota(jnp.int32, (per_row, per_row), 0)
            < lax.broadcasted_iota(jnp.int32, (per_row, per_row), 1)
        ).astype(jnp.float32)
        rank = jnp.dot(named, earlier, preferred_element_type=jnp.float32)
        slot = jnp.sum(rank * named, axis=0, keepdims=True)
        spot = owner * capacity + slot
        rows = lax.broadcasted_iota(jnp.int32, (owners * capacity, per_row), 0).astype(jnp.float32)
        chosen = (rows == spot).astype(jnp.float32)
        cut = (stations - 1) * keep
        wide = jnp.concatenate([chosen[:, :cut]] * 3 + [chosen[:, cut:]] * 3, axis=1)
        select[...] = wide.astype(jnp.bfloat16)

    def push(c, u, h):
        return jnp.concatenate(
            [weights[c * CHUNK + 2 * u + i, :, h * 128 : (h + 1) * 128] for i in range(2)], axis=0
        ).T

    def drop(c, u, h, tall):
        for k in range(128 // runs):
            turned[c * GROUP + u, pl.ds(h * (128 // runs) + k, runs, stride=8), :] = tall[
                k * runs : (k + 1) * runs
            ]

    tiles = [(u, h) for u in range(GROUP) for h in range(y_cells // 128)]

    def ready():
        pl.semaphore_wait(barrier, slab + owners - 2)
        for d in range(1, slab):
            id_copy(d).start()

    held = {}

    def plan_ids():
        for d in range(1, slab):
            id_copy(d).wait()

    def plan_rows():
        lane = lax.broadcasted_iota(jnp.int32, (stations, per_row), 1) >> log2(keep)
        line = lane == lax.broadcasted_iota(jnp.int32, (stations, per_row), 0)
        flat = []
        for d in range(slab):
            ids = kept[...] if d == 0 else others[d - 1]
            wide = jnp.where(line, jnp.concatenate([ids] * stations, axis=1), 0)
            one = wide[0:1]
            for s in range(1, stations):
                one = one + wide[s : s + 1]
            flat.append(one)
        flat = jnp.concatenate(flat, axis=0)
        j = lax.broadcasted_iota(jnp.int32, (slab, per_row), 0)
        j = lax.rem(me - j + slab, slab)
        first, second, f0, f1, back = row_plan(flat, j, me, slab, half, x_cells, y_cells)
        rows_v[0] = first
        rows_v[1] = second
        held["tall"] = [f0, f1, back, back]

    def plan_turn():
        tall = jnp.concatenate(held["tall"], axis=0)
        tall = jnp.concatenate([tall, jnp.zeros((4 * slab, 128 - per_row), jnp.float32)], axis=1)
        held["tall"] = tall.T

    def plan_scale(s, d):
        tall = held["tall"]
        side = lax.broadcasted_iota(jnp.int32, (keep, lanes), 1) < z_cells
        z_part = kernel_scale * (zed[0:1] + height[s])
        k = s * keep
        f0 = tall[k : k + keep, d : d + 1]
        f1 = tall[k : k + keep, slab + d : slab + d + 1]
        back = tall[k : k + keep, 2 * slab + d : 2 * slab + d + 1]
        scale_v[s, d * keep : (d + 1) * keep] = jnp.where(side, f0, f1) * z_part
        back_v[s, d * keep : (d + 1) * keep] = jnp.broadcast_to(back, (keep, lanes))

    def finish_y(s, tile):
        at = (s * rows_x + tile * 8) * 8
        values = tree([sums[pl.ds(at + i, 8, stride=8), :] for i in range(8)])
        values = values + [halves[pl.ds(at + i, 8, stride=8), :] for i in range(8)]
        for b in range(16):
            to = (tile * 8 + b // 2) * y_cells + (b % 2) * 8
            fields[s][pl.ds(to, 8), :] = values[b]

    def last_group(row):
        level = 0
        while row >= pyramid(pairs, level + 1):
            level = level + 1
        return min(pairs - 1, ((row - pyramid(pairs, level) + 1) << level) - 1) // GROUP

    def finished(g):
        ready_at = [max(last_group(8 * t + i) for i in range(8)) for t in range(rows_x // 8)]
        return [t for t, at in enumerate(ready_at) if at == g]

    def gather(s, k):
        d, i = k // keep, k % keep
        for n in range(2):
            to = taken if n == 0 else given
            to[s, 2 * k : 2 * k + 2, :] = fields[s][pl.ds(rows_s[n, d, s * keep + i], 2, stride=8), :]

    blocks = slab * keep

    def depth_dot(s):
        back, scale = back_v[s], scale_v[s]
        sides = []
        for t in range(2):
            mine = pl.ds(t, blocks, stride=2)
            sides.append((taken[s, mine, :] + back * given[s, mine, :]) * scale)
        held[s] = jnp.dot(
            pieces(jnp.concatenate(sides, axis=1)), signs[...], preferred_element_type=jnp.float32
        )

    def send(s):
        tall = held.pop(s)
        rows = (tall[2 * blocks :] + tall[blocks : 2 * blocks]) + tall[:blocks]
        rows = rows * z_norms(z_cells)[0:1]
        for d in range(slab):
            parts[s, d] = rows[d * keep : (d + 1) * keep]
        for d in range(1, slab):
            part_copy(s, d).start()

    def total(s):
        value = parts[s, 0]
        for d in range(1, slab):
            part_copy(s, d).wait()
            value = value + arrived[s, d - 1]
        return value

    far = 2 * lax.broadcasted_iota(jnp.int32, (GROUP, 8, lanes), 0)
    far = far.astype(jnp.float32) + jnp.where(
        lax.broadcasted_iota(jnp.int32, (GROUP, 8, lanes), 2) < z_cells, 0.5, 1.5
    )

    def evaluate(s, g, before_run):
        east = (me * x_local).astype(jnp.float32) - place[0, s] * x_cells

        def where(row, v):
            if v == 0:
                return sums, (s * rows_x + row) * 8
            if v == 1:
                return halves, (s * rows_x + row) * 8
            return fields[s], row * y_cells + v * 8

        def put(row, v, value):
            ref, at = where(row, v)
            ref[pl.ds(at, 8), :] = value

        def get(row, v):
            ref, at = where(row, v)
            return ref[pl.ds(at, 8), :]

        e = far + (east + float(2 * g * GROUP))
        easts = e * e

        def emit(v, wide):
            values = [wide[i] for i in range(GROUP)]
            level, at = 0, g * GROUP
            while True:
                for i, value in enumerate(values):
                    put(pyramid(pairs, level) + at + i, v, value)
                if len(values) == 1:
                    break
                values = [values[2 * i] + values[2 * i + 1] for i in range(len(values) // 2)]
                level, at = level + 1, at // 2
            value = values[0]
            while at & 1:
                value = get(pyramid(pairs, level) + at - 1, v) + value
                level, at = level + 1, at // 2
                put(pyramid(pairs, level) + at, v, value)

        stack = []
        for r in range(runs):
            before_run(r)
            inv = lax.rsqrt(table[s, r] + easts)
            w = turned[g * GROUP : (g + 1) * GROUP, r * 8 : r * 8 + 8, :]
            values = (w * inv) * (inv * inv)
            level, run = 0, r
            while stack and stack[-1][0] == level:
                _, other = stack.pop()
                level, run = level + 1, run >> 1
                emit((runs >> level) + run, other - values)
                values = other + values
            stack.append((level, values))
        emit(0, stack[0][1])

    class Phase:
        def __init__(self, order):
            self.order, self.steps, self.work = order, len(order) * runs, {}

        def at(self, step, f, *args):
            step = min(int(step), self.steps - 1)
            self.work.setdefault(step, []).append(functools.partial(f, *args))

        def over(self, items, start, stop):
            for n, item in enumerate(items):
                self.at((start + (stop - start) * n / len(items)) * self.steps, *item)

        def tiles(self):
            for i, (s, g) in enumerate(self.order):
                if g < groups - 1:
                    for n, t in enumerate(finished(g)):
                        self.at((i + 1) * runs + 2 + 8 * n, finish_y, s, t)

        def run(self):
            for s in sorted({s for s, _ in self.order}):
                heights(s)
            for i, (s, g) in enumerate(self.order):
                def before_run(r, i=i):
                    for f in self.work.get(i * runs + r, ()):
                        f()
                evaluate(s, g, before_run)

    def tiles_after(s):
        return [(finish_y, s, t) for t in finished(groups - 1)]

    def gathers(s):
        return [(gather, s, k) for k in range(blocks)]

    def push_later(c, u, h):
        held[c, u, h] = push(c, u, h)

    def drop_later(c, u, h):
        drop(c, u, h, held.pop((c, u, h)))

    w_copy(0).wait()
    for u, h in tiles:
        drop(0, u, h, push(0, u, h))

    first = Phase([(s, g) for g in range(groups) for s in range(2)])
    for g in range(groups - 1):
        start = 2 * g * runs
        first.at(start, lambda c: w_copy(c).wait(), g + 1)
        for n, (u, h) in enumerate(tiles):
            first.at(start + 5 * n, push_later, g + 1, u, h)
            first.at(start + 5 * n + 18, drop_later, g + 1, u, h)
    first.at(2 * runs, ready)
    first.tiles()
    first.run()

    second = Phase([(2, g) for g in range(groups)])
    second.over(tiles_after(0) + tiles_after(1), 0.0, 0.18)
    second.at(0.22 * second.steps, plan_ids)
    second.at(0.22 * second.steps, plan_rows)
    second.at(0.44 * second.steps, lambda: row_copy().start())
    second.at(0.44 * second.steps, plan_turn)
    second.over([(plan_scale, s, d) for s in range(stations) for d in range(slab)], 0.52, 0.70)
    second.at(0.70 * second.steps, lambda: row_copy().wait())
    second.over(gathers(0), 0.71, 0.99)
    second.tiles()
    second.run()

    third = Phase([(s, g) for s in range(3, stations) for g in range(groups)])
    third.over(tiles_after(2), 0.0, 0.1)
    third.at(0, depth_dot, 0)
    third.over(gathers(1), 0.02, 0.30)
    third.at(0.31 * third.steps, depth_dot, 1)
    third.over(gathers(2), 0.33, 0.62)
    third.at(0.50 * third.steps, send, 0)
    third.at(0.50 * third.steps, send, 1)
    third.at(0.64 * third.steps, depth_dot, 2)
    third.at(0.88 * third.steps, send, 2)
    third.tiles()
    third.run()

    for f, *args in tiles_after(3) + gathers(3):
        f(*args)
    depth_dot(3)
    send(3)
    choose()
    most = jnp.concatenate([total(s) for s in range(stations - 1)], axis=0)
    cut = 3 * (stations - 1) * keep
    early = jnp.dot(select[:, :cut], pieces(most), preferred_element_type=jnp.float32)
    late = jnp.dot(
        select[:, cut:], pieces(total(stations - 1)), preferred_element_type=jnp.float32
    )
    packed[...] = (early + late).reshape(packed.shape)
    for d in range(1, owners):
        out_copy(d).start()
    own = pltpu.make_async_copy(packed.at[q], out.at[q], own_sem)
    own.start()
    own.wait()
    for d in range(1, owners):
        out_copy(d).wait()


def local(station_place, station_height, cell_weight, kept, dest):
    slab = lax.axis_size("slab")
    owners = lax.axis_size("sta")
    x_local, y_cells, z_cells = cell_weight.shape
    stations = station_place.shape[0]
    keep = kept.shape[2]
    lanes = 2 * z_cells
    per_row = stations * keep
    capacity = max(2, 3 * per_row // owners)
    sizes = (slab, owners, stations, keep, x_local, y_cells, z_cells, capacity)
    dma = pltpu.SemaphoreType.DMA
    f32, i32 = jnp.float32, jnp.int32
    out = pl.pallas_call(
        functools.partial(whole_kernel, sizes),
        out_shape=pltpu.VMEM((owners, capacity, lanes), f32),
        in_specs=[pl.BlockSpec(memory_space=pl.ANY)] * 5,
        out_specs=pl.BlockSpec(memory_space=pl.ANY),
        scratch_shapes=[
            [pltpu.VMEM((x_local * y_cells, lanes), f32)] * stations,
            pltpu.VMEM((stations * x_local * 8, lanes), f32),
            pltpu.VMEM((stations * x_local * 8, lanes), f32),
            pltpu.SMEM((2, stations), f32),
            pltpu.SMEM((stations,), f32),
            pltpu.VMEM((stations, keep), i32),
            pltpu.VMEM((stations, 1, keep), i32),
            pltpu.VMEM((x_local, z_cells, y_cells), f32),
            pltpu.VMEM((x_local // 2, y_cells, lanes), f32),
            pltpu.VMEM((stations, y_cells // 8, 8, lanes), f32),
            pltpu.VMEM((owners * capacity, 3 * per_row), jnp.bfloat16),
            pltpu.VMEM((2 * lanes, lanes), jnp.bfloat16),
            pltpu.VMEM((slab - 1, stations, keep), i32),
            pltpu.VMEM((2, slab, per_row), i32),
            pltpu.SMEM((2, slab, per_row), i32),
            pltpu.VMEM((stations, slab * keep, lanes), f32),
            pltpu.VMEM((stations, slab * keep, lanes), f32),
            pltpu.VMEM((stations, 2 * slab * keep, lanes), f32),
            pltpu.VMEM((stations, 2 * slab * keep, lanes), f32),
            pltpu.VMEM((stations, slab, keep, lanes), f32),
            pltpu.VMEM((stations, slab - 1, keep, lanes), f32),
            pltpu.VMEM((owners, capacity, lanes), f32),
            dma((x_local // CHUNK,)),
            dma((4,)),
            dma,
            dma((slab - 1,)),
            dma((slab - 1,)),
            dma((stations, slab - 1)),
            dma((stations, slab - 1)),
            dma((owners - 1,)),
            dma((owners - 1,)),
            dma,
        ],
        compiler_params=pltpu.CompilerParams(
            collective_id=0, has_side_effects=True, vmem_limit_bytes=52_000_000
        ),
    )(
        *(
            pltpu.with_memory_space_constraint(a, pltpu.HBM)
            for a in (
                jnp.transpose(station_place),
                station_height,
                jnp.transpose(cell_weight, (0, 2, 1)),
                kept,
                jnp.transpose(dest, (0, 1, 3, 2)).reshape(stations, 1, keep),
            )
        )
    )
    return out.reshape(1, 1, owners, capacity, lanes)


def solution(mesh):
    placed = (
        P("sta", None),
        P("sta"),
        P("slab", None, None),
        P("slab", "sta", None),
        P("slab", "sta", None, None),
    )
    return jax.shard_map(
        local,
        mesh=mesh,
        in_specs=placed,
        out_specs=P("slab", "sta", None, None, None),
        check_vma=False,
    )
```

```python
import functools

import jax
import jax.numpy as jnp
from jax import lax
from jax.experimental import pallas as pl
from jax.experimental.pallas import tpu as pltpu
from jax.sharding import PartitionSpec as P

kernel_scale = 32.0
MESH = pl.DeviceIdType.MESH


def log2(n):
    return n.bit_length() - 1


def pyramid(pairs, level):
    return 2 * pairs - (2 * pairs >> level)


def row_plan(ids, j, me, slab, half, x_cells, y_cells):
    ls = log2(slab)
    pairs = x_cells // slab // 2
    a = ids >> log2(half)
    pair = j * half + (ids & (half - 1))
    total = pyramid(pairs, log2(pairs))
    first = jnp.full(a.shape, total, jnp.int32)
    second = jnp.full(a.shape, total, jnp.int32)
    factor = jnp.full(a.shape, x_cells ** -0.5, jnp.float32)
    turn = jnp.full(a.shape, 1.0, jnp.float32)
    back = jnp.full(a.shape, 0.0, jnp.float32)
    m = 1
    while m < x_cells:
        e = log2(m)
        at = a >= m
        k = a - m
        norm = (m / x_cells) ** 0.5
        if m >= slab:
            sh = e - ls
            mine = (k >> sh) == me
            here = k & ((1 << sh) - 1)
            factor = jnp.where(at, jnp.where(mine, norm, 0.0), factor)
            width = x_cells // m
            if width == 2:
                first = jnp.where(at, here, first)
                second = jnp.where(at, here, second)
                turn = jnp.where(at, -1.0, turn)
                back = jnp.where(at, 0.0, back)
            else:
                off = pyramid(pairs, log2(width) - 2)
                first = jnp.where(at, off + 2 * here, first)
                second = jnp.where(at, off + 2 * here + 1, second)
                back = jnp.where(at, -1.0, back)
        else:
            sh = ls - e
            mine = k == (me >> sh)
            sign = norm * (1 - 2 * ((me >> (sh - 1)) & 1)).astype(jnp.float32)
            factor = jnp.where(at, jnp.where(mine, sign, 0.0), factor)
        m = m * 2
    ynorm = jnp.full(a.shape, y_cells ** -0.5, jnp.float32)
    m = 1
    while m < y_cells // 2:
        ynorm = jnp.where(pair >= m, (2 * m / y_cells) ** 0.5, ynorm)
        m = m * 2

    def address(row):
        at = ((row & ~7) + pair) * y_cells + (row & 7)
        m = 16
        while m < y_cells:
            k = 2 * pair - m
            wide = m // 8
            spot = 8 * (wide + (k & (wide - 1))) + (k >> log2(wide))
            at = jnp.where(k >= 0, row * y_cells + spot, at)
            m = m * 2
        return at

    factor = factor * ynorm
    return address(first), address(second), factor, factor * turn, back


def z_signs(z_cells, t):
    z = lax.broadcasted_iota(jnp.int32, (2 * z_cells, 2 * z_cells), 0) & (z_cells - 1)
    lane = lax.broadcasted_iota(jnp.int32, (2 * z_cells, 2 * z_cells), 1)
    c = lane & (z_cells - 1)
    value = jnp.full(z.shape, 1.0, jnp.float32)
    m = 1
    while m < z_cells:
        w = log2(z_cells // m)
        k = c - m
        hit = (z >> w) == k
        up = ((z >> (w - 1)) & 1) == 0
        value = jnp.where(c >= m, jnp.where(hit, jnp.where(up, 1.0, -1.0), 0.0), value)
        m = m * 2
    return jnp.where((lane >> log2(z_cells)) == t, value, 0.0)


def z_norms(z_cells):
    c = lax.broadcasted_iota(jnp.int32, (8, 2 * z_cells), 1) & (z_cells - 1)
    norm = jnp.full(c.shape, z_cells ** -0.5, jnp.float32)
    m = 1
    while m < z_cells:
        norm = jnp.where(c >= m, (m / z_cells) ** 0.5, norm)
        m = m * 2
    return norm


def pieces(x):
    high = x.astype(jnp.bfloat16)
    rest = x - high.astype(jnp.float32)
    middle = rest.astype(jnp.bfloat16)
    low = (rest - middle.astype(jnp.float32)).astype(jnp.bfloat16)
    return jnp.concatenate([high, middle, low], axis=0)


def tree(values):
    out = [None] * len(values)
    while len(values) > 1:
        half = len(values) // 2
        for k in range(half):
            out[half + k] = values[2 * k] - values[2 * k + 1]
        values = [values[2 * k] + values[2 * k + 1] for k in range(half)]
    out[0] = values[0]
    return out


GROUP = 4
CHUNK = 2 * GROUP


def whole_kernel(
    sizes, place_h, height_h, w_hbm, kept_h, dest_h, out,
    fields, sums, halves, place, height, kept, dest,
    weights, turned, table, select, signs, others, rows_v, rows_s, scale_v, back_v,
    taken, given, parts, arrived, packed,
    w_sem, in_sem, row_sem, i_send, i_recv, s_send, s_recv, o_send, o_recv, own_sem,
):
    slab, owners, stations, keep, x_local, y_cells, z_cells, capacity = sizes
    lanes = 2 * z_cells
    pairs = x_local // 2
    rows_x = 2 * pairs
    groups = pairs // GROUP
    x_cells = x_local * slab
    half = y_cells // slab // 2
    per_row = stations * keep
    runs = y_cells // 8
    me, q = lax.axis_index("slab"), lax.axis_index("sta")
    zed = (lax.broadcasted_iota(jnp.int32, (8, lanes), 1) & (z_cells - 1)).astype(jnp.float32) + 0.5

    def before(d):
        return lax.rem(me - d + slab, slab)

    def id_copy(d):
        return pltpu.make_async_remote_copy(
            src_ref=kept,
            dst_ref=others.at[d - 1],
            send_sem=i_send.at[d - 1],
            recv_sem=i_recv.at[d - 1],
            device_id=(lax.rem(me + d, slab), q),
            device_id_type=MESH,
        )

    def part_copy(s, d):
        return pltpu.make_async_remote_copy(
            src_ref=parts.at[s, d],
            dst_ref=arrived.at[s, d - 1],
            send_sem=s_send.at[s, d - 1],
            recv_sem=s_recv.at[s, d - 1],
            device_id=(before(d), q),
            device_id_type=MESH,
        )

    def out_copy(d):
        to = lax.rem(q + d, owners)
        return pltpu.make_async_remote_copy(
            src_ref=packed.at[to],
            dst_ref=out.at[q],
            send_sem=o_send.at[d - 1],
            recv_sem=o_recv.at[d - 1],
            device_id=(me, to),
            device_id_type=MESH,
        )

    def row_copy():
        return pltpu.make_async_copy(rows_v, rows_s, row_sem)

    def w_copy(c):
        return pltpu.make_async_copy(
            w_hbm.at[pl.ds(c * CHUNK, CHUNK)], weights.at[pl.ds(c * CHUNK, CHUNK)], w_sem.at[c]
        )

    inputs = [
        pltpu.make_async_copy(a, b, in_sem.at[i])
        for i, (a, b) in enumerate(
            [(place_h, place), (height_h, height), (kept_h.at[0], kept), (dest_h, dest)]
        )
    ]
    with jax.named_scope("weights_in"):
        for copy in inputs:
            copy.start()
    for c in range(groups):
        w_copy(c).start()
    barrier = pltpu.get_barrier_semaphore()
    for d in range(1, slab):
        pl.semaphore_signal(
            barrier, inc=1, device_id=(lax.rem(me + d, slab), q), device_id_type=MESH
        )
    for d in range(1, owners):
        pl.semaphore_signal(
            barrier, inc=1, device_id=(me, lax.rem(q + d, owners)), device_id_type=MESH
        )
    with jax.named_scope("signs"):
        signs[...] = jnp.concatenate([z_signs(z_cells, 0), z_signs(z_cells, 1)], axis=0).astype(jnp.bfloat16)
    for copy in inputs:
        copy.wait()

    def heights(s):
        base = (lax.broadcasted_iota(jnp.int32, (8, lanes), 0) * runs).astype(jnp.float32) + 0.5
        depth = zed + height[s]
        square = depth * depth
        north = base - place[1, s] * y_cells
        for r in range(runs):
            n = north + float(r)
            table[s, r] = n * n + square

    def choose():
        owner = jnp.zeros((1, per_row), jnp.float32)
        for s in range(stations):
            spread = lax.broadcasted_iota(jnp.int32, (keep, per_row), 1) == (
                lax.broadcasted_iota(jnp.int32, (keep, per_row), 0) + s * keep
            )
            owner = owner + jnp.dot(
                dest[s].astype(jnp.float32), spread.astype(jnp.float32),
                preferred_element_type=jnp.float32,
            )
        names = lax.broadcasted_iota(jnp.int32, (owners, per_row), 0).astype(jnp.float32)
        named = (names == owner).astype(jnp.float32)
        earlier = (
            lax.broadcasted_iota(jnp.int32, (per_row, per_row), 0)
            < lax.broadcasted_iota(jnp.int32, (per_row, per_row), 1)
        ).astype(jnp.float32)
        rank = jnp.dot(named, earlier, preferred_element_type=jnp.float32)
        slot = jnp.sum(rank * named, axis=0, keepdims=True)
        spot = owner * capacity + slot
        rows = lax.broadcasted_iota(jnp.int32, (owners * capacity, per_row), 0).astype(jnp.float32)
        chosen = (rows == spot).astype(jnp.float32)
        cut = (stations - 1) * keep
        wide = jnp.concatenate([chosen[:, :cut]] * 3 + [chosen[:, cut:]] * 3, axis=1)
        select[...] = wide.astype(jnp.bfloat16)

    def push(c, u, h):
        return jnp.concatenate(
            [weights[c * CHUNK + 2 * u + i, :, h * 128 : (h + 1) * 128] for i in range(2)], axis=0
        ).T

    def drop(c, u, h, tall):
        for k in range(128 // runs):
            turned[c * GROUP + u, pl.ds(h * (128 // runs) + k, runs, stride=8), :] = tall[
                k * runs : (k + 1) * runs
            ]

    tiles = [(u, h) for u in range(GROUP) for h in range(y_cells // 128)]

    def ready():
        pl.semaphore_wait(barrier, slab + owners - 2)
        for d in range(1, slab):
            id_copy(d).start()

    held = {}

    def plan_ids():
        for d in range(1, slab):
            id_copy(d).wait()

    def plan_rows():
        lane = lax.broadcasted_iota(jnp.int32, (stations, per_row), 1) >> log2(keep)
        line = lane == lax.broadcasted_iota(jnp.int32, (stations, per_row), 0)
        flat = []
        for d in range(slab):
            ids = kept[...] if d == 0 else others[d - 1]
            wide = jnp.where(line, jnp.concatenate([ids] * stations, axis=1), 0)
            one = wide[0:1]
            for s in range(1, stations):
                one = one + wide[s : s + 1]
            flat.append(one)
        flat = jnp.concatenate(flat, axis=0)
        j = lax.broadcasted_iota(jnp.int32, (slab, per_row), 0)
        j = lax.rem(me - j + slab, slab)
        first, second, f0, f1, back = row_plan(flat, j, me, slab, half, x_cells, y_cells)
        rows_v[0] = first
        rows_v[1] = second
        held["tall"] = [f0, f1, back, back]

    def plan_turn():
        tall = jnp.concatenate(held["tall"], axis=0)
        tall = jnp.concatenate([tall, jnp.zeros((4 * slab, 128 - per_row), jnp.float32)], axis=1)
        held["tall"] = tall.T

    def plan_scale(s, d):
        tall = held["tall"]
        side = lax.broadcasted_iota(jnp.int32, (keep, lanes), 1) < z_cells
        z_part = kernel_scale * (zed[0:1] + height[s])
        k = s * keep
        f0 = tall[k : k + keep, d : d + 1]
        f1 = tall[k : k + keep, slab + d : slab + d + 1]
        back = tall[k : k + keep, 2 * slab + d : 2 * slab + d + 1]
        scale_v[s, d * keep : (d + 1) * keep] = jnp.where(side, f0, f1) * z_part
        back_v[s, d * keep : (d + 1) * keep] = jnp.broadcast_to(back, (keep, lanes))

    def finish_y(s, tile):
        at = (s * rows_x + tile * 8) * 8
        values = tree([sums[pl.ds(at + i, 8, stride=8), :] for i in range(8)])
        values = values + [halves[pl.ds(at + i, 8, stride=8), :] for i in range(8)]
        for b in range(16):
            to = (tile * 8 + b // 2) * y_cells + (b % 2) * 8
            fields[s][pl.ds(to, 8), :] = values[b]

    def last_group(row):
        level = 0
        while row >= pyramid(pairs, level + 1):
            level = level + 1
        return min(pairs - 1, ((row - pyramid(pairs, level) + 1) << level) - 1) // GROUP

    def finished(g):
        ready_at = [max(last_group(8 * t + i) for i in range(8)) for t in range(rows_x // 8)]
        return [t for t, at in enumerate(ready_at) if at == g]

    def gather(s, k):
        d, i = k // keep, k % keep
        for n in range(2):
            to = taken if n == 0 else given
            to[s, 2 * k : 2 * k + 2, :] = fields[s][pl.ds(rows_s[n, d, s * keep + i], 2, stride=8), :]

    blocks = slab * keep

    def depth_dot(s):
        back, scale = back_v[s], scale_v[s]
        sides = []
        for t in range(2):
            mine = pl.ds(t, blocks, stride=2)
            sides.append((taken[s, mine, :] + back * given[s, mine, :]) * scale)
        held[s] = jnp.dot(
            pieces(jnp.concatenate(sides, axis=1)), signs[...], preferred_element_type=jnp.float32
        )

    def send(s):
        tall = held.pop(s)
        rows = (tall[2 * blocks :] + tall[blocks : 2 * blocks]) + tall[:blocks]
        rows = rows * z_norms(z_cells)[0:1]
        for d in range(slab):
            parts[s, d] = rows[d * keep : (d + 1) * keep]
        for d in range(1, slab):
            part_copy(s, d).start()

    def total(s):
        value = parts[s, 0]
        for d in range(1, slab):
            part_copy(s, d).wait()
            value = value + arrived[s, d - 1]
        return value

    far = 2 * lax.broadcasted_iota(jnp.int32, (GROUP, 8, lanes), 0)
    far = far.astype(jnp.float32) + jnp.where(
        lax.broadcasted_iota(jnp.int32, (GROUP, 8, lanes), 2) < z_cells, 0.5, 1.5
    )

    def evaluate(s, g, before_run):
        east = (me * x_local).astype(jnp.float32) - place[0, s] * x_cells

        def where(row, v):
            if v == 0:
                return sums, (s * rows_x + row) * 8
            if v == 1:
                return halves, (s * rows_x + row) * 8
            return fields[s], row * y_cells + v * 8

        def put(row, v, value):
            ref, at = where(row, v)
            ref[pl.ds(at, 8), :] = value

        def get(row, v):
            ref, at = where(row, v)
            return ref[pl.ds(at, 8), :]

        e = far + (east + float(2 * g * GROUP))
        easts = e * e

        def emit(v, wide):
            values = [wide[i] for i in range(GROUP)]
            level, at = 0, g * GROUP
            while True:
                for i, value in enumerate(values):
                    put(pyramid(pairs, level) + at + i, v, value)
                if len(values) == 1:
                    break
                values = [values[2 * i] + values[2 * i + 1] for i in range(len(values) // 2)]
                level, at = level + 1, at // 2
            value = values[0]
            while at & 1:
                value = get(pyramid(pairs, level) + at - 1, v) + value
                level, at = level + 1, at // 2
                put(pyramid(pairs, level) + at, v, value)

        stack = []
        for r in range(runs):
            before_run(r)
            inv = lax.rsqrt(table[s, r] + easts)
            w = turned[g * GROUP : (g + 1) * GROUP, r * 8 : r * 8 + 8, :]
            values = (w * inv) * (inv * inv)
            level, run = 0, r
            while stack and stack[-1][0] == level:
                _, other = stack.pop()
                level, run = level + 1, run >> 1
                emit((runs >> level) + run, other - values)
                values = other + values
            stack.append((level, values))
        emit(0, stack[0][1])

    class Phase:
        def __init__(self, order):
            self.order, self.steps, self.work = order, len(order) * runs, {}

        def at(self, step, f, *args):
            step = min(int(step), self.steps - 1)
            self.work.setdefault(step, []).append(functools.partial(f, *args))

        def over(self, items, start, stop):
            for n, item in enumerate(items):
                self.at((start + (stop - start) * n / len(items)) * self.steps, *item)

        def tiles(self):
            for i, (s, g) in enumerate(self.order):
                if g < groups - 1:
                    for n, t in enumerate(finished(g)):
                        self.at((i + 1) * runs + 2 + 8 * n, finish_y, s, t)

        def run(self):
            for s in sorted({s for s, _ in self.order}):
                heights(s)
            for i, (s, g) in enumerate(self.order):
                def before_run(r, i=i):
                    for f in self.work.get(i * runs + r, ()):
                        f()
                evaluate(s, g, before_run)

    def tiles_after(s):
        return [(finish_y, s, t) for t in finished(groups - 1)]

    def gathers(s):
        return [(gather, s, k) for k in range(blocks)]

    def push_later(c, u, h):
        held[c, u, h] = push(c, u, h)

    def drop_later(c, u, h):
        drop(c, u, h, held.pop((c, u, h)))

    with jax.named_scope("first_turn"):
        w_copy(0).wait()
        for u, h in tiles:
            drop(0, u, h, push(0, u, h))

    first = Phase([(s, g) for g in range(groups) for s in range(2)])
    for g in range(groups - 1):
        start = 2 * g * runs
        first.at(start, lambda c: w_copy(c).wait(), g + 1)
        for n, (u, h) in enumerate(tiles):
            first.at(start + 5 * n, push_later, g + 1, u, h)
            first.at(start + 5 * n + 18, drop_later, g + 1, u, h)
    first.at(2 * runs, ready)
    first.tiles()
    with jax.named_scope("stations_0_1"):
        first.run()

    second = Phase([(2, g) for g in range(groups)])
    second.over(tiles_after(0) + tiles_after(1), 0.0, 0.18)
    second.at(0.22 * second.steps, plan_ids)
    second.at(0.22 * second.steps, plan_rows)
    second.at(0.44 * second.steps, lambda: row_copy().start())
    second.at(0.44 * second.steps, plan_turn)
    second.over([(plan_scale, s, d) for s in range(stations) for d in range(slab)], 0.52, 0.70)
    second.at(0.70 * second.steps, lambda: row_copy().wait())
    second.over(gathers(0), 0.71, 0.99)
    second.tiles()
    with jax.named_scope("station_2"):
        second.run()

    third = Phase([(s, g) for s in range(3, stations) for g in range(groups)])
    third.over(tiles_after(2), 0.0, 0.1)
    third.at(0, depth_dot, 0)
    third.over(gathers(1), 0.02, 0.30)
    third.at(0.31 * third.steps, depth_dot, 1)
    third.over(gathers(2), 0.33, 0.62)
    third.at(0.50 * third.steps, send, 0)
    third.at(0.50 * third.steps, send, 1)
    third.at(0.64 * third.steps, depth_dot, 2)
    third.at(0.88 * third.steps, send, 2)
    third.tiles()
    with jax.named_scope("station_3"):
        third.run()

    with jax.named_scope("last_send"):
        for f, *args in tiles_after(3) + gathers(3):
            f(*args)
        depth_dot(3)
        send(3)
        choose()
    with jax.named_scope("early_pack"):
        most = jnp.concatenate([total(s) for s in range(stations - 1)], axis=0)
        cut = 3 * (stations - 1) * keep
        early = jnp.dot(select[:, :cut], pieces(most), preferred_element_type=jnp.float32)
    with jax.named_scope("late_pack"):
        late = jnp.dot(
            select[:, cut:], pieces(total(stations - 1)), preferred_element_type=jnp.float32
        )
        packed[...] = (early + late).reshape(packed.shape)
    for d in range(1, owners):
        out_copy(d).start()
    own = pltpu.make_async_copy(packed.at[q], out.at[q], own_sem)
    own.start()
    own.wait()
    for d in range(1, owners):
        out_copy(d).wait()


def local(station_place, station_height, cell_weight, kept, dest):
    slab = lax.axis_size("slab")
    owners = lax.axis_size("sta")
    x_local, y_cells, z_cells = cell_weight.shape
    stations = station_place.shape[0]
    keep = kept.shape[2]
    lanes = 2 * z_cells
    per_row = stations * keep
    capacity = max(2, 3 * per_row // owners)
    sizes = (slab, owners, stations, keep, x_local, y_cells, z_cells, capacity)
    dma = pltpu.SemaphoreType.DMA
    f32, i32 = jnp.float32, jnp.int32
    out = pl.pallas_call(
        functools.partial(whole_kernel, sizes),
        out_shape=pltpu.VMEM((owners, capacity, lanes), f32),
        in_specs=[pl.BlockSpec(memory_space=pl.ANY)] * 5,
        out_specs=pl.BlockSpec(memory_space=pl.ANY),
        scratch_shapes=[
            [pltpu.VMEM((x_local * y_cells, lanes), f32)] * stations,
            pltpu.VMEM((stations * x_local * 8, lanes), f32),
            pltpu.VMEM((stations * x_local * 8, lanes), f32),
            pltpu.SMEM((2, stations), f32),
            pltpu.SMEM((stations,), f32),
            pltpu.VMEM((stations, keep), i32),
            pltpu.VMEM((stations, 1, keep), i32),
            pltpu.VMEM((x_local, z_cells, y_cells), f32),
            pltpu.VMEM((x_local // 2, y_cells, lanes), f32),
            pltpu.VMEM((stations, y_cells // 8, 8, lanes), f32),
            pltpu.VMEM((owners * capacity, 3 * per_row), jnp.bfloat16),
            pltpu.VMEM((2 * lanes, lanes), jnp.bfloat16),
            pltpu.VMEM((slab - 1, stations, keep), i32),
            pltpu.VMEM((2, slab, per_row), i32),
            pltpu.SMEM((2, slab, per_row), i32),
            pltpu.VMEM((stations, slab * keep, lanes), f32),
            pltpu.VMEM((stations, slab * keep, lanes), f32),
            pltpu.VMEM((stations, 2 * slab * keep, lanes), f32),
            pltpu.VMEM((stations, 2 * slab * keep, lanes), f32),
            pltpu.VMEM((stations, slab, keep, lanes), f32),
            pltpu.VMEM((stations, slab - 1, keep, lanes), f32),
            pltpu.VMEM((owners, capacity, lanes), f32),
            dma((x_local // CHUNK,)),
            dma((4,)),
            dma,
            dma((slab - 1,)),
            dma((slab - 1,)),
            dma((stations, slab - 1)),
            dma((stations, slab - 1)),
            dma((owners - 1,)),
            dma((owners - 1,)),
            dma,
        ],
        compiler_params=pltpu.CompilerParams(
            collective_id=0, has_side_effects=True, vmem_limit_bytes=52_000_000
        ),
    )(
        *(
            pltpu.with_memory_space_constraint(a, pltpu.HBM)
            for a in (
                jnp.transpose(station_place),
                station_height,
                jnp.transpose(cell_weight, (0, 2, 1)),
                kept,
                jnp.transpose(dest, (0, 1, 3, 2)).reshape(stations, 1, keep),
            )
        )
    )
    return out.reshape(1, 1, owners, capacity, lanes)


def solution(mesh):
    placed = (
        P("sta", None),
        P("sta"),
        P("slab", None, None),
        P("slab", "sta", None),
        P("slab", "sta", None, None),
    )
    return jax.shard_map(
        local,
        mesh=mesh,
        in_specs=placed,
        out_specs=P("slab", "sta", None, None, None),
        check_vma=False,
    )
```
